512 devices in a mesh: ka: 16 (over y_hi, x), band: 32 (over y_lo, z, core).
Axes of the slice: x: 4, y: 8 (y_hi: 4, y_lo: 2; y = y_hi * 2 + y_lo), z: 8, core: 2. Of those that a mesh axis runs over, the one named last changes fastest.
Arguments:
- targets: bfloat16 [16, 32, 24, 24, 128], P('ka', 'band'), may hold values from -6 to 6
- occupied: bfloat16 [16, 64, 24, 24, 128], P('ka', 'band'), may hold values from -6 to 6
- wavevectors: int32 [16, 3], replicated, may hold values from 0 to 3
- umklapp: int32 [16, 2, 3], P('ka'), may hold values from -1 to 1
- owners: int32 [16, 2, 2], P('ka'), may hold values from 0 to 31
Outputs:
- exchange: bfloat16 [16, 32, 24, 24, 128], P('ka', 'band')
The draws below stay inside these ranges and needn't reach their ends.
All inputs are finite; a program needn't handle non-finite values.
Results may differ from the reference program's by a relative error of at most 0.017.
Values may be sent and summed in bfloat16 or wider, within the bound.
No kernel may reach another device: no remote copies, remote signals or barrier semaphores. Data moves between devices by JAX's collectives and lax.ppermute only.
A program may use at most 64 MiB of HBM per device.

```python
import math
import jax
import jax.numpy as jnp
from jax import lax

NX = 64
NY = 24
NZ = 24
OCC_DEV = 2
STEPS = 2
KGRID = 4
KPTS = 16
BANDS = 32
OCC_BANDS = 64
N_BAND = 32


def place_ends(values, stream_key, smallest, largest):
    longest = values.shape.index(max(values.shape))
    spots = []
    for shift in (0, 1):
        where = [jax.random.randint(jax.random.fold_in(stream_key, axis), (), 0, length) for axis, length in enumerate(values.shape)]
        where[longest] = (where[longest] + shift) % values.shape[longest]
        spots.append(tuple(where))
    return values.at[spots[0]].set(smallest).at[spots[1]].set(largest)


def steps_of(own_key, dims, cuts, least, top_value):
    def one(position, parts):
        heights = jax.random.uniform(jax.random.fold_in(jax.random.fold_in(own_key, 6), position), (parts,), jnp.float32, least / len(cuts), top_value / len(cuts))
        return jnp.repeat(jnp.exp(heights), dims[position] // parts).reshape((-1,) + (1,) * (len(dims) - position - 1))

    factor_of = one(*cuts[0])
    for cut in cuts[1:]:
        factor_of = factor_of * one(*cut)
    return factor_of


def normal_values(stream_key, dims, width, limit, cuts=(), kind=jnp.bfloat16):
    loudness = steps_of(stream_key, dims, cuts, -0.22, 0.18) if cuts else 1.0
    values = jax.random.normal(stream_key, dims, jnp.float32) * width * loudness
    return jnp.minimum(jnp.maximum(values, -limit), limit).astype(kind)


def setup_inputs(seed: int = 0) -> dict:
    splits = jax.random.split(jax.random.key(seed), 6)
    targets = normal_values(splits[0], (KPTS, BANDS, NY, NZ, 2 * NX), 1.0, 6.0, ((0, 16), (1, 32)))
    occupied = normal_values(splits[1], (KPTS, OCC_BANDS, NY, NZ, 2 * NX), 1.0, 6.0, ((0, 16), (1, 32)))
    wavevectors = place_ends(jax.random.randint(splits[2], (KPTS, 3), 0, KGRID), jax.random.fold_in(splits[2], 1), 0, KGRID - 1).astype(jnp.int32)
    umklapp = place_ends(jax.random.randint(splits[3], (KPTS, STEPS, 3), -1, 2), jax.random.fold_in(splits[3], 1), -1, 1).astype(jnp.int32)
    owners = place_ends(jax.random.randint(splits[4], (KPTS, STEPS, OCC_DEV), 0, N_BAND), jax.random.fold_in(splits[4], 1), 0, N_BAND - 1).astype(jnp.int32)
    return dict(targets=targets, occupied=occupied, wavevectors=wavevectors, umklapp=umklapp, owners=owners)


screening_sq = 0.16
spacing = 0.25
prefactor = -0.5


def tables(length):
    indices = jnp.arange(length, dtype=jnp.int32)
    products = (indices[:, None] * indices[None, :]) % length
    angles = products.astype(jnp.float32) * (2.0 * math.pi / length)
    return jnp.cos(angles), jnp.sin(angles)


def last_matrix(length, sign_value):
    cosine, sine_table = tables(length)
    upper_rows = jnp.concatenate([cosine, -sign_value * sine_table], axis=1)
    bottom = jnp.concatenate([sign_value * sine_table, cosine], axis=1)
    return jnp.concatenate([upper_rows, bottom], axis=0).astype(jnp.bfloat16)


def stacked_table(length):
    cosine, sine_table = tables(length)
    return jnp.concatenate([cosine, sine_table], axis=0).astype(jnp.bfloat16)


def along_axis(grid_values, spec, length, sign_value, axis_pos):
    both = jnp.einsum(spec, stacked_table(length).astype(jnp.float32), grid_values.astype(jnp.float32), precision=lax.Precision.HIGHEST)
    cos_part = lax.slice_in_dim(both, 0, length, axis=axis_pos)
    sin_part = lax.slice_in_dim(both, length, 2 * length, axis=axis_pos)
    half_width = both.shape[-1] // 2
    swapped = jnp.concatenate([sin_part[..., half_width:], sin_part[..., :half_width]], axis=-1)
    half_sign = jnp.concatenate([jnp.ones((half_width,), jnp.float32), -jnp.ones((half_width,), jnp.float32)])
    return (cos_part + sign_value * half_sign * swapped).astype(jnp.bfloat16)


def fourier(grid_values, sign_value):
    last_width = grid_values.shape[-1]
    flattened = grid_values.reshape(-1, last_width)
    moved = jnp.dot(flattened.astype(jnp.float32), last_matrix(last_width // 2, sign_value).astype(jnp.float32), precision=lax.Precision.HIGHEST)
    grid_values = moved.astype(jnp.bfloat16).reshape(grid_values.shape)
    grid_values = along_axis(grid_values, "vy,byzc->bvzc", grid_values.shape[1], sign_value, 1)
    grid_values = along_axis(grid_values, "vz,byzc->byvc", grid_values.shape[2], sign_value, 2)
    return grid_values


def coulomb(shift_vec, grid_x, grid_y, grid_z):
    squares = []
    for axis_pos, length in ((0, grid_x), (1, grid_y), (2, grid_z)):
        indices = jnp.arange(length, dtype=jnp.int32)
        signed = jnp.where(indices * 2 < length, indices, indices - length)
        wavenumber = (2.0 * math.pi / (length * spacing)) * (signed.astype(jnp.float32) + shift_vec[axis_pos])
        squares.append(wavenumber * wavenumber)
    square_x = jnp.concatenate([squares[0], squares[0]])
    total_sq = squares[1][:, None, None] + squares[2][None, :, None] + square_x[None, None, :] + screening_sq
    return 4.0 * math.pi / total_sq


def pair_density(visitor, resident):
    half_width = visitor.shape[-1] // 2
    visit_re = visitor[..., :half_width].astype(jnp.float32)
    visit_im = visitor[..., half_width:].astype(jnp.float32)
    res_re = resident[..., :half_width].astype(jnp.float32)
    res_im = resident[..., half_width:].astype(jnp.float32)
    real_part = visit_re * res_re + visit_im * res_im
    imag_part = visit_re * res_im - visit_im * res_re
    return jnp.concatenate([real_part, imag_part], axis=-1).astype(jnp.bfloat16)


def apply_potential(visitor, potential):
    half_width = visitor.shape[-1] // 2
    visit_re = visitor[..., :half_width].astype(jnp.float32)
    visit_im = visitor[..., half_width:].astype(jnp.float32)
    pot_re = potential[..., :half_width].astype(jnp.float32)
    pot_im = potential[..., half_width:].astype(jnp.float32)
    real_part = visit_re * pot_re - visit_im * pot_im
    imag_part = visit_re * pot_im + visit_im * pot_re
    return jnp.concatenate([real_part, imag_part], axis=-1)


def exchange_term(visitor, resident, kernel, cells):
    density = pair_density(visitor, resident)
    spectrum = fourier(density, 1.0)
    screened = (spectrum.astype(jnp.float32) * kernel * (1.0 / cells)).astype(jnp.bfloat16)
    potential = fourier(screened, -1.0)
    return apply_potential(visitor, potential)


def reference(targets, occupied, wavevectors, umklapp, owners):
    k_total = targets.shape[0]
    grid_y, grid_z, last_width = targets.shape[2], targets.shape[3], targets.shape[4]
    grid_x = last_width // 2
    cells = float(grid_x * grid_y * grid_z)

    def one_point(point_index):
        resident = lax.dynamic_index_in_dim(targets, point_index, 0, keepdims=False)
        own_coords = lax.dynamic_index_in_dim(wavevectors, point_index, 0, keepdims=False)
        shifts = lax.dynamic_index_in_dim(umklapp, point_index, 0, keepdims=False)
        choosers = lax.dynamic_index_in_dim(owners, point_index, 0, keepdims=False)
        accumulated = jnp.zeros(resident.shape, jnp.float32)
        for section_index in range(1, STEPS + 1):
            visit_index = ((point_index - section_index) % k_total).astype(jnp.int32)
            visiting = lax.dynamic_index_in_dim(occupied, visit_index, 0, keepdims=False)
            visit_coords = lax.dynamic_index_in_dim(wavevectors, visit_index, 0, keepdims=False)
            shift_vec = (own_coords - visit_coords).astype(jnp.float32) / KGRID + shifts[section_index - 1].astype(jnp.float32)
            kernel = coulomb(shift_vec, grid_x, grid_y, grid_z)
            for slot_index in range(OCC_DEV):
                chosen = (choosers[section_index - 1, slot_index] * OCC_DEV + slot_index).astype(jnp.int32)
                visitor = lax.dynamic_index_in_dim(visiting, chosen, 0, keepdims=False)
                accumulated = accumulated + exchange_term(visitor, resident, kernel, cells)
        return (prefactor * accumulated).astype(jnp.bfloat16)

    return lax.map(one_point, jnp.arange(k_total, dtype=jnp.int32))
```

```python
import math

import jax
import jax.numpy as jnp
import ml_dtypes
import numpy as np
from jax import lax
from jax.experimental import pallas as pl
from jax.experimental.pallas import tpu as pltpu
from jax.sharding import PartitionSpec as P

OCC_DEV = 2
STEPS = 2
KGRID = 4

screening_sq = 0.16
spacing = 0.25
prefactor = -0.5

PIECE = 40
PIECES = 16
LANES = 128


def shift_ka(block, distance):
    size = lax.axis_size("ka")
    return lax.ppermute(block, "ka", [(i, (i + distance) % size) for i in range(size)])


def band_groups():
    along_z = [[y * 16 + z * 2 + c for z in range(8)] for y in range(2) for c in range(2)]
    along_yc = [[y * 16 + z * 2 + c for y in range(2) for c in range(2)] for z in range(8)]
    return along_z, along_yc


def rounded_tables(length):
    indices = np.arange(length)
    angles = (indices[:, None] * indices[None, :] % length) * (2.0 * math.pi / length)
    rounded = lambda t: t.astype(np.float32).astype(ml_dtypes.bfloat16).astype(np.float64)
    return rounded(np.cos(angles)), rounded(np.sin(angles))


def plane_table(grid_y, grid_z):
    cos_y, sin_y = rounded_tables(grid_y)
    cos_z, sin_z = rounded_tables(grid_z)
    cosine = np.kron(cos_y, cos_z) - np.kron(sin_y, sin_z)
    sine = np.kron(sin_y, cos_z) + np.kron(cos_y, sin_z)
    return np.concatenate([cosine, sine], axis=1).astype(np.float32).astype(ml_dtypes.bfloat16)


def line_table(grid_x, sign):
    cosine, sine = rounded_tables(grid_x)
    re_in = np.concatenate([cosine, -sign * sine], axis=1)
    im_in = np.concatenate([sign * sine, cosine], axis=1)
    straight = np.concatenate([re_in, im_in], axis=0)
    turned = np.concatenate([sign * straight[:, grid_x:], -sign * straight[:, :grid_x]], axis=1)
    return np.concatenate([straight, turned], axis=1).astype(np.float32).astype(ml_dtypes.bfloat16)


def coulomb(shift_vec, grid_x, grid_y, grid_z):
    squares = []
    for axis_pos, length in ((0, grid_x), (1, grid_y), (2, grid_z)):
        indices = jnp.arange(length, dtype=jnp.int32)
        signed = jnp.where(indices * 2 < length, indices, indices - length)
        wavenumber = (
            2.0 * math.pi / (length * spacing) * (signed.astype(jnp.float32) + shift_vec[axis_pos])
        )
        squares.append(wavenumber * wavenumber)
    square_x = jnp.concatenate([squares[0], squares[0]])
    total_sq = (
        squares[1][:, None, None]
        + squares[2][None, :, None]
        + square_x[None, None, :]
        + screening_sq
    )
    return 4.0 * math.pi / total_sq


def exchange_kernel(pieces, psi, table, forward, inverse, kern, out, direct, cross, stack):
    rows, half = out.shape[0], LANES // 2
    terms = STEPS * OCC_DEV
    left = lax.broadcasted_iota(jnp.int32, (1, LANES), 1) < half

    for piece in range(PIECES):
        first = piece * PIECE
        count = min(PIECE, rows - first)
        if count <= 0:
            continue
        own = psi[pl.ds(first, count), :].astype(jnp.float32)
        own_turned = pltpu.roll(own, half, 1)
        for term in range(terms):
            s, r = divmod(term, OCC_DEV)
            z, c = divmod(piece, 2)
            phi = pieces[r * 2 + c, z, s].astype(jnp.float32)[:count]
            phi_turned = pltpu.roll(phi, half, 1)
            a = jnp.where(left, phi, phi_turned)
            b = jnp.where(left, -phi_turned, phi)
            direct[term, pl.ds(first, count), :] = a
            cross[term, pl.ds(first, count), :] = b
            density = (a * own - b * own_turned).astype(jnp.bfloat16)
            both = jnp.dot(density, forward[...], preferred_element_type=jnp.float32)
            lane = term * LANES
            stack[pl.ds(first, count), pl.ds(lane, LANES)] = both[:, :LANES]
            stack[pl.ds(rows + first, count), pl.ds(lane, LANES)] = both[:, LANES:]

    spectrum = jnp.dot(
        table[...], stack[...].astype(jnp.bfloat16), preferred_element_type=jnp.float32
    )
    for term in range(terms):
        lane = term * LANES
        screened = (spectrum[:, lane : lane + LANES] * kern[term // OCC_DEV]).astype(jnp.bfloat16)
        both = jnp.dot(screened, inverse[...], preferred_element_type=jnp.float32)
        stack[pl.ds(0, rows), pl.ds(lane, LANES)] = both[:, :LANES]
        stack[pl.ds(rows, rows), pl.ds(lane, LANES)] = both[:, LANES:]
    potential = jnp.dot(
        table[...], stack[...].astype(jnp.bfloat16), preferred_element_type=jnp.float32
    )
    total = jnp.zeros((rows, LANES), jnp.float32)
    for term in range(terms):
        lane = term * LANES
        pot = potential[:, lane : lane + LANES]
        total += direct[term] * pot + cross[term] * pltpu.roll(pot, half, 1)
    out[...] = (prefactor * total).astype(out.dtype)


def apply_exchange(pieces, psi, kern, grid_x, grid_y, grid_z):
    rows = grid_y * grid_z
    terms = STEPS * OCC_DEV
    vmem = pl.BlockSpec(memory_space=pltpu.VMEM)
    return pl.pallas_call(
        exchange_kernel,
        out_shape=jax.ShapeDtypeStruct((rows, LANES), jnp.bfloat16),
        in_specs=[vmem] * 6,
        out_specs=vmem,
        scratch_shapes=[
            pltpu.VMEM((terms, rows, LANES), jnp.float32),
            pltpu.VMEM((terms, rows, LANES), jnp.float32),
            pltpu.VMEM((2 * rows, terms * LANES), jnp.float32),
        ],
        compiler_params=pltpu.CompilerParams(vmem_limit_bytes=40 * 1024 * 1024),
    )(
        pieces,
        psi,
        jnp.asarray(plane_table(grid_y, grid_z)),
        jnp.asarray(line_table(grid_x, 1.0)),
        jnp.asarray(line_table(grid_x, -1.0)),
        kern,
    )


def local(targets, occupied, wavevectors, umklapp, owners):
    resident = targets[0, 0]
    grid_y, grid_z, last_width = resident.shape
    grid_x = last_width // 2
    rows = grid_y * grid_z
    cells = float(grid_x * rows)
    ka_position = lax.axis_index("ka")
    k_total = lax.axis_size("ka")
    slot = lax.axis_index("band") // PIECES
    along_z, along_yc = band_groups()

    wanted = [shift_ka(owners[0, s - 1], -s) for s in range(1, STEPS + 1)]

    flat = occupied[0].reshape(OCC_DEV, rows, last_width)
    flat = jnp.pad(flat, ((0, 0), (0, PIECE * PIECES - rows), (0, 0)))
    flat = flat.reshape(OCC_DEV * PIECES, PIECE, last_width)
    spread = lax.all_to_all(flat, "band", 0, 0, tiled=True)

    chosen = []
    for s in range(1, STEPS + 1):
        owner = lax.dynamic_index_in_dim(wanted[s - 1], slot, 0, keepdims=False)
        piece = lax.dynamic_index_in_dim(spread, owner, 0, keepdims=False)
        chosen.append(shift_ka(piece, s))
    mine = jnp.stack(chosen)

    column = jnp.broadcast_to(mine[None], (8,) + mine.shape)
    column = lax.all_to_all(column, "band", 0, 0, tiled=True, axis_index_groups=along_z)
    pieces = lax.all_gather(column, "band", axis_index_groups=along_yc)

    own_coords = lax.dynamic_index_in_dim(wavevectors, ka_position, 0, keepdims=False)
    kernels = []
    for s in range(1, STEPS + 1):
        visit_coords = lax.dynamic_index_in_dim(
            wavevectors, (ka_position - s) % k_total, 0, keepdims=False
        )
        shift_vec = (own_coords - visit_coords).astype(jnp.float32) / KGRID + umklapp[
            0, s - 1
        ].astype(jnp.float32)
        kernels.append(coulomb(shift_vec, grid_x, grid_y, grid_z) * (1.0 / cells))
    kern = jnp.stack(kernels).reshape(STEPS, rows, last_width)

    result = apply_exchange(
        pieces, resident.reshape(rows, last_width), kern, grid_x, grid_y, grid_z
    )
    return result.reshape((1, 1) + resident.shape)


def solution(mesh):
    placed = (
        P("ka", "band", None, None, None),
        P("ka", "band", None, None, None),
        P(),
        P("ka", None, None),
        P("ka", None, None),
    )
    return jax.shard_map(
        local,
        mesh=mesh,
        in_specs=placed,
        out_specs=P("ka", "band", None, None, None),
        check_vma=False,
    )
```

```python
import math

import jax
import jax.numpy as jnp
import ml_dtypes
import numpy as np
from jax import lax
from jax.experimental import pallas as pl
from jax.experimental.pallas import tpu as pltpu
from jax.sharding import PartitionSpec as P


OCC_DEV = 2
STEPS = 2
KGRID = 4

screening_sq = 0.16
spacing = 0.25
prefactor = -0.5

LANES = 128


def shift_ka_by_core(block, sign):
    n_ka, n_band = lax.axis_size("ka"), lax.axis_size("band")
    route = []
    for k in range(n_ka):
        for b in range(n_band):
            to = (k + sign * (1 + b % 2)) % n_ka
            route.append((k * n_band + b, to * n_band + b))
    return lax.ppermute(block, ("ka", "band"), route)


def band_groups():
    along_yz = [[yz * 2 + c for yz in range(16)] for c in range(2)]
    cores = [[yz * 2 + c for c in range(2)] for yz in range(16)]
    return along_yz, cores


def rounded_tables(length):
    indices = np.arange(length)
    angles = (indices[:, None] * indices[None, :] % length) * (2.0 * math.pi / length)
    rounded = lambda t: t.astype(np.float32).astype(ml_dtypes.bfloat16).astype(np.float64)
    return rounded(np.cos(angles)), rounded(np.sin(angles))


def plane_table(grid_y, grid_z):
    cos_y, sin_y = rounded_tables(grid_y)
    cos_z, sin_z = rounded_tables(grid_z)
    cosine = np.kron(cos_y, cos_z) - np.kron(sin_y, sin_z)
    sine = np.kron(sin_y, cos_z) + np.kron(cos_y, sin_z)
    return np.concatenate([cosine, sine], axis=1).astype(np.float32).astype(ml_dtypes.bfloat16)


def line_table(grid_x, sign):
    cosine, sine = rounded_tables(grid_x)
    re_in = np.concatenate([cosine, -sign * sine], axis=1)
    im_in = np.concatenate([sign * sine, cosine], axis=1)
    straight = np.concatenate([re_in, im_in], axis=0)
    turned = np.concatenate([sign * straight[:, grid_x:], -sign * straight[:, :grid_x]], axis=1)
    return np.concatenate([straight, turned], axis=1).astype(np.float32).astype(ml_dtypes.bfloat16)


def coulomb_kernel(wavevectors, umklapp, out):
    steps, grid_y, grid_z, width = out.shape
    grid_x = width // 2
    cells = float(grid_x * grid_y * grid_z)
    k = lax.axis_index("ka")
    k_total = lax.axis_size("ka")

    def square(index, length, shift):
        signed = jnp.where(index * 2 < length, index, index - length).astype(jnp.float32)
        wavenumber = 2.0 * math.pi / (length * spacing) * (signed + shift)
        return wavenumber * wavenumber

    lane = lax.broadcasted_iota(jnp.int32, (grid_z, width), 1)
    index_x = jnp.where(lane < grid_x, lane, lane - grid_x)
    index_z = lax.broadcasted_iota(jnp.int32, (grid_z, width), 0)
    for s in range(steps):
        visit = lax.rem(k + (k_total - s - 1), k_total)
        shift = [
            (wavevectors[k, a] - wavevectors[visit, a]).astype(jnp.float32) / KGRID
            + umklapp[0, s, a].astype(jnp.float32)
            for a in range(3)
        ]
        plane = square(index_x, grid_x, shift[0]) + square(index_z, grid_z, shift[2])
        plane = plane + screening_sq
        for y in range(grid_y):
            signed_y = float(y if 2 * y < grid_y else y - grid_y)
            wave_y = 2.0 * math.pi / (grid_y * spacing) * (signed_y + shift[1])
            out[s, y] = (4.0 * math.pi / cells) / (plane + wave_y * wave_y)


def coulomb(wavevectors, umklapp, grid_x, grid_y, grid_z):
    smem = pl.BlockSpec(memory_space=pltpu.SMEM)
    return pl.pallas_call(
        coulomb_kernel,
        out_shape=jax.ShapeDtypeStruct((STEPS, grid_y, grid_z, 2 * grid_x), jnp.float32),
        in_specs=[smem, smem],
        out_specs=pl.BlockSpec(memory_space=pltpu.VMEM),
    )(wavevectors, umklapp)


def exchange_kernel(visitors, psi, table, forward, inverse, kern, out, direct, cross, stack):
    rows, half = out.shape[0], LANES // 2
    terms = STEPS * OCC_DEV
    left = lax.broadcasted_iota(jnp.int32, (1, LANES), 1) < half

    chunk = 144
    for term in range(terms):
        lane = term * LANES
        for first in range(0, rows, chunk):
            own = psi[pl.ds(first, chunk), :].astype(jnp.float32)
            own_turned = pltpu.roll(own, half, 1)
            phi = visitors[term, pl.ds(first, chunk), :].astype(jnp.float32)
            phi_turned = pltpu.roll(phi, half, 1)
            a = jnp.where(left, phi, phi_turned)
            b = jnp.where(left, -phi_turned, phi)
            direct[term, pl.ds(first, chunk), :] = a
            cross[term, pl.ds(first, chunk), :] = b
            density = (a * own - b * own_turned).astype(jnp.bfloat16)
            both = jnp.dot(density, forward[...], preferred_element_type=jnp.float32)
            both = both.astype(jnp.bfloat16)
            stack[pl.ds(first, chunk), pl.ds(lane, LANES)] = both[:, :LANES]
            stack[pl.ds(rows + first, chunk), pl.ds(lane, LANES)] = both[:, LANES:]

    spectrum = jnp.dot(
        table[...], stack[...], preferred_element_type=jnp.float32
    )
    for term in range(terms):
        lane = term * LANES
        screened = (spectrum[:, lane : lane + LANES] * kern[term // OCC_DEV]).astype(jnp.bfloat16)
        both = jnp.dot(screened, inverse[...], preferred_element_type=jnp.float32)
        both = both.astype(jnp.bfloat16)
        stack[pl.ds(0, rows), pl.ds(lane, LANES)] = both[:, :LANES]
        stack[pl.ds(rows, rows), pl.ds(lane, LANES)] = both[:, LANES:]
    potential = jnp.dot(
        table[...], stack[...], preferred_element_type=jnp.float32
    )
    total = jnp.zeros((rows, LANES), jnp.float32)
    for term in range(terms):
        lane = term * LANES
        pot = potential[:, lane : lane + LANES]
        total += direct[term] * pot + cross[term] * pltpu.roll(pot, half, 1)
    out[...] = (prefactor * total).astype(out.dtype)


def apply_exchange(visitors, psi, kern, grid_x, grid_y, grid_z):
    rows = grid_y * grid_z
    terms = STEPS * OCC_DEV
    vmem = pl.BlockSpec(memory_space=pltpu.VMEM)
    return pl.pallas_call(
        exchange_kernel,
        out_shape=jax.ShapeDtypeStruct((rows, LANES), jnp.bfloat16),
        in_specs=[vmem] * 6,
        out_specs=vmem,
        scratch_shapes=[
            pltpu.VMEM((terms, rows, LANES), jnp.float32),
            pltpu.VMEM((terms, rows, LANES), jnp.float32),
            pltpu.VMEM((2 * rows, terms * LANES), jnp.bfloat16),
        ],
        compiler_params=pltpu.CompilerParams(vmem_limit_bytes=40 * 1024 * 1024),
    )(
        visitors,
        psi,
        jnp.asarray(plane_table(grid_y, grid_z)),
        jnp.asarray(line_table(grid_x, 1.0)),
        jnp.asarray(line_table(grid_x, -1.0)),
        kern,
    )


def exchange(targets, occupied, wavevectors, umklapp, owners):
    resident = targets[0, 0]
    grid_y, grid_z, last_width = resident.shape
    grid_x = last_width // 2
    rows = grid_y * grid_z
    band = lax.axis_index("band")
    core, slot = band % 2, band // 16
    along_yz, cores = band_groups()
    n_yz = len(cores)

    flat = occupied[0].reshape(n_yz, OCC_DEV * rows // n_yz, last_width)
    spread = lax.all_to_all(flat, "band", 0, 0, tiled=True, axis_index_groups=along_yz)
    spread = lax.all_gather(spread, "band", axis_index_groups=cores)

    wanted = shift_ka_by_core(owners[0], -1)
    owner = lax.dynamic_slice(wanted, (core, slot), (1, 1))[0, 0]
    spread = spread.reshape((2 * n_yz,) + flat.shape[1:])
    chosen = lax.dynamic_index_in_dim(spread, owner % 2 * n_yz + owner // 2, 0, keepdims=False)
    mine = shift_ka_by_core(chosen, 1)

    column = jnp.broadcast_to(mine[None], (n_yz,) + mine.shape)
    column = lax.all_to_all(column, "band", 0, 0, tiled=True, axis_index_groups=along_yz)
    kern = coulomb(wavevectors, umklapp, grid_x, grid_y, grid_z)
    visitors = lax.all_gather(column, "band", axis_index_groups=cores)
    visitors = visitors.reshape(STEPS * OCC_DEV, rows, last_width)

    result = apply_exchange(
        visitors,
        resident.reshape(rows, last_width),
        kern.reshape(STEPS, rows, last_width),
        grid_x,
        grid_y,
        grid_z,
    )
    return result.reshape((1, 1) + resident.shape)


def solution(mesh):
    placed = (
        P("ka", "band", None, None, None),
        P("ka", "band", None, None, None),
        P(),
        P("ka", None, None),
        P("ka", None, None),
    )
    return jax.shard_map(
        exchange,
        mesh=mesh,
        in_specs=placed,
        out_specs=P("ka", "band", None, None, None),
        check_vma=False,
    )
```

```python
import math

import jax
import jax.numpy as jnp
import ml_dtypes
import numpy as np
from jax import lax
from jax.experimental import pallas as pl
from jax.experimental.pallas import tpu as pltpu
from jax.sharding import PartitionSpec as P


OCC_DEV = 2
STEPS = 2
KGRID = 4

screening_sq = 0.16
spacing = 0.25
prefactor = -0.5

LANES = 128


def shift_ka_by_core(block, sign):
    n_ka, n_band = lax.axis_size("ka"), lax.axis_size("band")
    route = []
    for k in range(n_ka):
        for b in range(n_band):
            to = (k + sign * (1 + b % 2)) % n_ka
            route.append((k * n_band + b, to * n_band + b))
    return lax.ppermute(block, ("ka", "band"), route)


def band_groups():
    along_yz = [[yz * 2 + c for yz in range(16)] for c in range(2)]
    cores = [[yz * 2 + c for c in range(2)] for yz in range(16)]
    return along_yz, cores


def rounded_tables(length):
    indices = np.arange(length)
    angles = (indices[:, None] * indices[None, :] % length) * (2.0 * math.pi / length)
    rounded = lambda t: t.astype(np.float32).astype(ml_dtypes.bfloat16).astype(np.float64)
    return rounded(np.cos(angles)), rounded(np.sin(angles))


def plane_table(grid_y, grid_z):
    cos_y, sin_y = rounded_tables(grid_y)
    cos_z, sin_z = rounded_tables(grid_z)
    cosine = np.kron(cos_y, cos_z) - np.kron(sin_y, sin_z)
    sine = np.kron(sin_y, cos_z) + np.kron(cos_y, sin_z)
    return np.concatenate([cosine, sine], axis=1).astype(np.float32).astype(ml_dtypes.bfloat16)


def line_table(grid_x, sign):
    cosine, sine = rounded_tables(grid_x)
    re_in = np.concatenate([cosine, -sign * sine], axis=1)
    im_in = np.concatenate([sign * sine, cosine], axis=1)
    straight = np.concatenate([re_in, im_in], axis=0)
    turned = np.concatenate([sign * straight[:, grid_x:], -sign * straight[:, :grid_x]], axis=1)
    return np.concatenate([straight, turned], axis=1).astype(np.float32).astype(ml_dtypes.bfloat16)


def coulomb_kernel(wavevectors, umklapp, out):
    steps, grid_y, grid_z, width = out.shape
    grid_x = width // 2
    cells = float(grid_x * grid_y * grid_z)
    k = lax.axis_index("ka")
    k_total = lax.axis_size("ka")

    def square(index, length, shift):
        signed = jnp.where(index * 2 < length, index, index - length).astype(jnp.float32)
        wavenumber = 2.0 * math.pi / (length * spacing) * (signed + shift)
        return wavenumber * wavenumber

    lane = lax.broadcasted_iota(jnp.int32, (grid_z, width), 1)
    index_x = jnp.where(lane < grid_x, lane, lane - grid_x)
    index_z = lax.broadcasted_iota(jnp.int32, (grid_z, width), 0)
    for s in range(steps):
        visit = lax.rem(k + (k_total - s - 1), k_total)
        shift = [
            (wavevectors[a, k] - wavevectors[a, visit]).astype(jnp.float32) / KGRID
            + umklapp[0, s, a].astype(jnp.float32)
            for a in range(3)
        ]
        plane = square(index_x, grid_x, shift[0]) + square(index_z, grid_z, shift[2])
        plane = plane + screening_sq
        for y in range(grid_y):
            signed_y = float(y if 2 * y < grid_y else y - grid_y)
            wave_y = 2.0 * math.pi / (grid_y * spacing) * (signed_y + shift[1])
            out[s, y] = (4.0 * math.pi / cells) / (plane + wave_y * wave_y)


def coulomb(wavevectors, umklapp, grid_x, grid_y, grid_z):
    smem = pl.BlockSpec(memory_space=pltpu.SMEM)
    return pl.pallas_call(
        coulomb_kernel,
        out_shape=jax.ShapeDtypeStruct((STEPS, grid_y, grid_z, 2 * grid_x), jnp.float32),
        in_specs=[smem, smem],
        out_specs=pl.BlockSpec(memory_space=pltpu.VMEM),
    )(wavevectors.T, umklapp)


def exchange_kernel(visitors, psi, table, forward, inverse, kern, out, direct, cross, stack):
    rows, half = out.shape[0], LANES // 2
    terms = STEPS * OCC_DEV
    left = lax.broadcasted_iota(jnp.int32, (1, LANES), 1) < half

    chunk = 144
    for term in range(terms):
        lane = term * LANES
        for first in range(0, rows, chunk):
            own = psi[pl.ds(first, chunk), :].astype(jnp.float32)
            own_turned = pltpu.roll(own, half, 1)
            phi = visitors[term, pl.ds(first, chunk), :].astype(jnp.float32)
            phi_turned = pltpu.roll(phi, half, 1)
            a = jnp.where(left, phi, phi_turned)
            b = jnp.where(left, -phi_turned, phi)
            direct[term, pl.ds(first, chunk), :] = a
            cross[term, pl.ds(first, chunk), :] = b
            density = (a * own - b * own_turned).astype(jnp.bfloat16)
            both = jnp.dot(density, forward[...], preferred_element_type=jnp.float32)
            both = both.astype(jnp.bfloat16)
            stack[pl.ds(first, chunk), pl.ds(lane, LANES)] = both[:, :LANES]
            stack[pl.ds(rows + first, chunk), pl.ds(lane, LANES)] = both[:, LANES:]

    spectrum = jnp.dot(
        table[...], stack[...], preferred_element_type=jnp.float32
    )
    for term in range(terms):
        lane = term * LANES
        screened = (spectrum[:, lane : lane + LANES] * kern[term // OCC_DEV]).astype(jnp.bfloat16)
        both = jnp.dot(screened, inverse[...], preferred_element_type=jnp.float32)
        both = both.astype(jnp.bfloat16)
        stack[pl.ds(0, rows), pl.ds(lane, LANES)] = both[:, :LANES]
        stack[pl.ds(rows, rows), pl.ds(lane, LANES)] = both[:, LANES:]
    potential = jnp.dot(
        table[...], stack[...], preferred_element_type=jnp.float32
    )
    total = jnp.zeros((rows, LANES), jnp.float32)
    for term in range(terms):
        lane = term * LANES
        pot = potential[:, lane : lane + LANES]
        total += direct[term] * pot + cross[term] * pltpu.roll(pot, half, 1)
    out[...] = (prefactor * total).astype(out.dtype)


def apply_exchange(visitors, psi, kern, grid_x, grid_y, grid_z):
    rows = grid_y * grid_z
    terms = STEPS * OCC_DEV
    vmem = pl.BlockSpec(memory_space=pltpu.VMEM)
    return pl.pallas_call(
        exchange_kernel,
        out_shape=jax.ShapeDtypeStruct((rows, LANES), jnp.bfloat16),
        in_specs=[vmem] * 6,
        out_specs=vmem,
        scratch_shapes=[
            pltpu.VMEM((terms, rows, LANES), jnp.float32),
            pltpu.VMEM((terms, rows, LANES), jnp.float32),
            pltpu.VMEM((2 * rows, terms * LANES), jnp.bfloat16),
        ],
        compiler_params=pltpu.CompilerParams(vmem_limit_bytes=40 * 1024 * 1024),
    )(
        visitors,
        psi,
        jnp.asarray(plane_table(grid_y, grid_z)),
        jnp.asarray(line_table(grid_x, 1.0)),
        jnp.asarray(line_table(grid_x, -1.0)),
        kern,
    )


def exchange(targets, occupied, wavevectors, umklapp, owners):
    resident = targets[0, 0]
    grid_y, grid_z, last_width = resident.shape
    grid_x = last_width // 2
    rows = grid_y * grid_z
    band = lax.axis_index("band")
    core, slot = band % 2, band // 16
    along_yz, cores = band_groups()
    n_yz = len(cores)

    flat = occupied[0].reshape(n_yz, OCC_DEV * rows // n_yz, last_width)
    spread = lax.all_to_all(flat, "band", 0, 0, tiled=True, axis_index_groups=along_yz)
    spread = lax.all_gather(spread, "band", axis_index_groups=cores)

    wanted = shift_ka_by_core(owners[0], -1)
    kern = coulomb(wavevectors, umklapp, grid_x, grid_y, grid_z)
    owner = lax.dynamic_slice(wanted, (core, slot), (1, 1), allow_negative_indices=False)[0, 0]
    spread = spread.reshape((2 * n_yz,) + flat.shape[1:])
    place = jnp.bitwise_and(owner, 1) * n_yz + lax.shift_right_logical(owner, 1)
    chosen = lax.dynamic_slice(
        spread, (place, 0, 0), (1,) + flat.shape[1:], allow_negative_indices=False
    )[0]
    mine = shift_ka_by_core(chosen, 1)

    column = jnp.broadcast_to(mine[None], (n_yz,) + mine.shape)
    column = lax.all_to_all(column, "band", 0, 0, tiled=True, axis_index_groups=along_yz)
    visitors = lax.all_gather(column, "band", axis_index_groups=cores)
    visitors = visitors.reshape(STEPS * OCC_DEV, rows, last_width)

    result = apply_exchange(
        visitors,
        resident.reshape(rows, last_width),
        kern.reshape(STEPS, rows, last_width),
        grid_x,
        grid_y,
        grid_z,
    )
    return result.reshape((1, 1) + resident.shape)


def solution(mesh):
    placed = (
        P("ka", "band", None, None, None),
        P("ka", "band", None, None, None),
        P(),
        P("ka", None, None),
        P("ka", None, None),
    )
    return jax.shard_map(
        exchange,
        mesh=mesh,
        in_specs=placed,
        out_specs=P("ka", "band", None, None, None),
        check_vma=False,
    )
```

```python
import functools
import math

import jax
import jax.numpy as jnp
import ml_dtypes
import numpy as np
from jax import lax
from jax.experimental import pallas as pl
from jax.experimental.pallas import tpu as pltpu
from jax.sharding import PartitionSpec as P


OCC_DEV = 2
STEPS = 2
KGRID = 4

screening_sq = 0.16
spacing = 0.25
prefactor = -0.5

LANES = 128


def shift_ka_by_core(block, sign):
    n_ka, n_band = lax.axis_size("ka"), lax.axis_size("band")
    route = []
    for k in range(n_ka):
        for b in range(n_band):
            to = (k + sign * (1 + b % 2)) % n_ka
            route.append((k * n_band + b, to * n_band + b))
    return lax.ppermute(block, ("ka", "band"), route)


def band_groups():
    along_yz = [[yz * 2 + c for yz in range(16)] for c in range(2)]
    cores = [[yz * 2 + c for c in range(2)] for yz in range(16)]
    return along_yz, cores


def rounded_tables(length):
    indices = np.arange(length)
    angles = (indices[:, None] * indices[None, :] % length) * (2.0 * math.pi / length)
    rounded = lambda t: t.astype(np.float32).astype(ml_dtypes.bfloat16).astype(np.float64)
    return rounded(np.cos(angles)), rounded(np.sin(angles))


def half_plane(grid_y, grid_z):
    rows = np.arange(grid_y * grid_z)
    opposite = (-(rows // grid_z)) % grid_y * grid_z + (-(rows % grid_z)) % grid_z
    chosen = rows[rows <= opposite]
    return chosen, opposite[chosen], (opposite[chosen] != chosen).astype(np.float32)


def half_padded(grid_y, grid_z):
    return -(-len(half_plane(grid_y, grid_z)[0]) // 64) * 64


def plane_tables(grid_y, grid_z):
    cos_y, sin_y = rounded_tables(grid_y)
    cos_z, sin_z = rounded_tables(grid_z)
    chosen = half_plane(grid_y, grid_z)[0]
    rows, half = grid_y * grid_z, half_padded(grid_y, grid_z)
    width = 2 * half
    there = np.zeros((2, half, width), np.float32)
    there[0, : len(chosen), :rows] = (np.kron(cos_y, cos_z) - np.kron(sin_y, sin_z))[chosen]
    there[1, : len(chosen), :rows] = (np.kron(sin_y, cos_z) + np.kron(cos_y, sin_z))[chosen]
    back = there[:, :, :rows].transpose(2, 0, 1).reshape(rows, 2 * half)
    return np.concatenate([there.reshape(2 * half, width), back]).astype(ml_dtypes.bfloat16)


def plane_frequencies(grid_y, grid_z):
    chosen, opposite, differ = half_plane(grid_y, grid_z)
    table = np.zeros((half_padded(grid_y, grid_z), 8), np.float32)
    for column, (which, length) in enumerate(
        [
            (chosen // grid_z, grid_y),
            (chosen % grid_z, grid_z),
            (opposite // grid_z, grid_y),
            (opposite % grid_z, grid_z),
        ]
    ):
        table[: len(chosen), column] = np.where(which * 2 < length, which, which - length)
    table[: len(chosen), 4] = differ
    return table


def line_table(grid_x, sign):
    cosine, sine = rounded_tables(grid_x)
    re_in = np.concatenate([cosine, -sign * sine], axis=1)
    im_in = np.concatenate([sign * sine, cosine], axis=1)
    straight = np.concatenate([re_in, im_in], axis=0)
    turned = np.concatenate([sign * straight[:, grid_x:], -sign * straight[:, :grid_x]], axis=1)
    return np.concatenate([straight, turned], axis=1).astype(np.float32).astype(ml_dtypes.bfloat16)


def coulomb_kernel(grid, wavevectors, umklapp, frequencies, out):
    grid_x, grid_y, grid_z = grid
    width = out.shape[-1]
    cells = float(grid_x * grid_y * grid_z)
    k = lax.axis_index("ka")
    k_total = lax.axis_size("ka")

    def square(signed, length, shift):
        wavenumber = 2.0 * math.pi / (length * spacing) * (signed + shift)
        return wavenumber * wavenumber

    lane = lax.broadcasted_iota(jnp.int32, (1, width), 1)
    index_x = jnp.where(lane < grid_x, lane, lane - grid_x)
    signed_x = jnp.where(index_x * 2 < grid_x, index_x, index_x - grid_x).astype(jnp.float32)
    for s in range(out.shape[0]):
        visit = lax.rem(k + (k_total - s - 1), k_total)
        shift = [
            (wavevectors[a, k] - wavevectors[a, visit]).astype(jnp.float32) / KGRID
            + umklapp[0, s, a].astype(jnp.float32)
            for a in range(3)
        ]
        line = square(signed_x, grid_x, shift[0])
        kern = []
        for column in (0, 2):
            plane = square(frequencies[:, column : column + 1], grid_y, shift[1]) + square(
                frequencies[:, column + 1 : column + 2], grid_z, shift[2]
            )
            kern.append((4.0 * math.pi / cells) / (plane + line + screening_sq))
        opposite = kern[1] * frequencies[:, 4:5]
        out[s, 0] = kern[0] + opposite
        out[s, 1] = kern[0] - opposite


def coulomb(wavevectors, umklapp, grid_x, grid_y, grid_z):
    smem = pl.BlockSpec(memory_space=pltpu.SMEM)
    vmem = pl.BlockSpec(memory_space=pltpu.VMEM)
    half = half_padded(grid_y, grid_z)
    return pl.pallas_call(
        functools.partial(coulomb_kernel, (grid_x, grid_y, grid_z)),
        out_shape=jax.ShapeDtypeStruct((STEPS, 2, half, 2 * grid_x), jnp.float32),
        in_specs=[smem, smem, vmem],
        out_specs=vmem,
    )(wavevectors.T, umklapp, jnp.asarray(plane_frequencies(grid_y, grid_z)))


def exchange_kernel(
    visitors, psi, planes, lines, kern, out, dense, given, even, odd, pair, stack, plane
):
    rows, turn = out.shape[0], LANES // 2
    width = planes.shape[1]
    half = width // 2
    terms = STEPS * OCC_DEV
    left = lax.broadcasted_iota(jnp.int32, (1, LANES), 1) < turn
    chunk = 96

    def lanes(term):
        return pl.ds(term * LANES, LANES)

    given[:, pl.ds(rows, width - rows), :] = jnp.zeros(
        (2, width - rows, terms * LANES), given.dtype
    )
    for first in range(0, rows, chunk):
        own = psi[pl.ds(first, chunk), :].astype(jnp.float32)
        turned = pltpu.roll(own, turn, 1)
        with_phi = jnp.where(left, own, -turned)
        with_turned = jnp.where(left, turned, own)
        for term in range(terms):
            phi = visitors[term, pl.ds(first, chunk), :].astype(jnp.float32)
            density = phi * with_phi + pltpu.roll(phi, turn, 1) * with_turned
            dense[pl.ds(term * rows + first, chunk), :] = density.astype(jnp.bfloat16)
    for term in range(terms):
        both = jnp.dot(
            dense[pl.ds(term * rows, rows), :],
            lines[:, : 2 * LANES],
            preferred_element_type=jnp.float32,
        ).astype(jnp.bfloat16)
        given[0, pl.ds(0, rows), lanes(term)] = both[:, :LANES]
        given[1, pl.ds(0, rows), lanes(term)] = both[:, LANES:]

    even[...] = jnp.dot(planes[:half], given[0], preferred_element_type=jnp.float32)
    odd[...] = jnp.dot(planes[half:width], given[1], preferred_element_type=jnp.float32)
    for term in range(terms):
        total, differ = kern[term // OCC_DEV, 0], kern[term // OCC_DEV, 1]
        e, o = even[:, lanes(term)], odd[:, lanes(term)]
        pair[0, pl.ds(term * half, half), :] = (e * total + o * differ).astype(jnp.bfloat16)
        pair[1, pl.ds(term * half, half), :] = (e * differ + o * total).astype(jnp.bfloat16)
    for part in range(2):
        turned = jnp.dot(
            pair[part],
            lines[:, (2 + part) * LANES : (3 + part) * LANES],
            preferred_element_type=jnp.float32,
        ).astype(jnp.bfloat16)
        for term in range(terms):
            stack[pl.ds(part * half, half), lanes(term)] = turned[term * half : (term + 1) * half]

    plane[...] = jnp.dot(planes[width:], stack[...], preferred_element_type=jnp.float32)
    for first in range(0, rows, chunk):
        straight = crossed = None
        for term in range(terms):
            phi = visitors[term, pl.ds(first, chunk), :].astype(jnp.float32)
            potential = plane[pl.ds(first, chunk), lanes(term)]
            one, two = phi * potential, pltpu.roll(phi, turn, 1) * potential
            straight = one if term == 0 else straight + one
            crossed = two if term == 0 else crossed + two
        total = jnp.where(
            left, straight - pltpu.roll(straight, turn, 1), crossed + pltpu.roll(crossed, turn, 1)
        )
        out[pl.ds(first, chunk), :] = (prefactor * total).astype(out.dtype)


def apply_exchange(visitors, psi, kern, grid_x, grid_y, grid_z):
    rows = grid_y * grid_z
    terms = STEPS * OCC_DEV
    planes = plane_tables(grid_y, grid_z)
    lines = np.concatenate([line_table(grid_x, 1.0), line_table(grid_x, -1.0)], axis=1)
    width = planes.shape[1]
    half = width // 2
    vmem = pl.BlockSpec(memory_space=pltpu.VMEM)
    return pl.pallas_call(
        exchange_kernel,
        out_shape=jax.ShapeDtypeStruct((rows, LANES), jnp.bfloat16),
        in_specs=[vmem] * 5,
        out_specs=vmem,
        scratch_shapes=[
            pltpu.VMEM((terms * rows, LANES), jnp.bfloat16),
            pltpu.VMEM((2, width, terms * LANES), jnp.bfloat16),
            pltpu.VMEM((half, terms * LANES), jnp.float32),
            pltpu.VMEM((half, terms * LANES), jnp.float32),
            pltpu.VMEM((2, terms * half, LANES), jnp.bfloat16),
            pltpu.VMEM((2 * half, terms * LANES), jnp.bfloat16),
            pltpu.VMEM((rows, terms * LANES), jnp.float32),
        ],
        compiler_params=pltpu.CompilerParams(vmem_limit_bytes=16 * 1024 * 1024),
    )(
        visitors,
        psi,
        jnp.asarray(planes),
        jnp.asarray(lines),
        kern,
    )


def exchange(targets, occupied, wavevectors, umklapp, owners):
    resident = targets[0, 0]
    grid_y, grid_z, last_width = resident.shape
    grid_x = last_width // 2
    rows = grid_y * grid_z
    band = lax.axis_index("band")
    core, slot = band % 2, band // 16
    along_yz, cores = band_groups()
    n_yz = len(cores)

    flat = occupied[0].reshape(n_yz, OCC_DEV * rows // n_yz, last_width)
    spread = lax.all_to_all(flat, "band", 0, 0, tiled=True, axis_index_groups=along_yz)
    spread = lax.all_gather(spread, "band", axis_index_groups=cores)

    wanted = shift_ka_by_core(owners[0], -1)
    owner = lax.dynamic_slice(wanted, (core, slot), (1, 1), allow_negative_indices=False)[0, 0]
    spread = spread.reshape((2 * n_yz,) + flat.shape[1:])
    place = jnp.bitwise_and(owner, 1) * n_yz + lax.shift_right_logical(owner, 1)
    chosen = lax.dynamic_slice(
        spread, (place, 0, 0), (1,) + flat.shape[1:], allow_negative_indices=False
    )[0]
    mine = shift_ka_by_core(chosen, 1)

    kern = coulomb(wavevectors, umklapp, grid_x, grid_y, grid_z)
    column = jnp.broadcast_to(mine[None], (n_yz,) + mine.shape)
    column = lax.all_to_all(column, "band", 0, 0, tiled=True, axis_index_groups=along_yz)
    visitors = lax.all_gather(column, "band", axis_index_groups=cores)
    visitors = visitors.reshape(STEPS * OCC_DEV, rows, last_width)

    result = apply_exchange(
        visitors,
        resident.reshape(rows, last_width),
        kern,
        grid_x,
        grid_y,
        grid_z,
    )
    return result.reshape((1, 1) + resident.shape)


def solution(mesh):
    placed = (
        P("ka", "band", None, None, None),
        P("ka", "band", None, None, None),
        P(),
        P("ka", None, None),
        P("ka", None, None),
    )
    return jax.shard_map(
        exchange,
        mesh=mesh,
        in_specs=placed,
        out_specs=P("ka", "band", None, None, None),
        check_vma=False,
    )
```

```python
import functools
import math

import jax
import jax.numpy as jnp
import ml_dtypes
import numpy as np
from jax import lax
from jax.experimental import pallas as pl
from jax.experimental.pallas import tpu as pltpu
from jax.sharding import PartitionSpec as P


OCC_DEV = 2
STEPS = 2
KGRID = 4

screening_sq = 0.16
spacing = 0.25
prefactor = -0.5

LANES = 128


def shift_ka_by_core(block, sign):
    n_ka, n_band = lax.axis_size("ka"), lax.axis_size("band")
    route = []
    for k in range(n_ka):
        for b in range(n_band):
            to = (k + sign * (1 + b % 2)) % n_ka
            route.append((k * n_band + b, to * n_band + b))
    return lax.ppermute(block, ("ka", "band"), route)


def band_groups():
    along_yz = [[yz * 2 + c for yz in range(16)] for c in range(2)]
    cores = [[yz * 2 + c for c in range(2)] for yz in range(16)]
    return along_yz, cores


def rounded_tables(length):
    indices = np.arange(length)
    angles = (indices[:, None] * indices[None, :] % length) * (2.0 * math.pi / length)
    rounded = lambda t: t.astype(np.float32).astype(ml_dtypes.bfloat16).astype(np.float64)
    return rounded(np.cos(angles)), rounded(np.sin(angles))


def half_plane(grid_y, grid_z):
    rows = np.arange(grid_y * grid_z)
    opposite = (-(rows // grid_z)) % grid_y * grid_z + (-(rows % grid_z)) % grid_z
    chosen = rows[rows <= opposite]
    return chosen, opposite[chosen], (opposite[chosen] != chosen).astype(np.float32)


def half_padded(grid_y, grid_z):
    return -(-len(half_plane(grid_y, grid_z)[0]) // 64) * 64


def plane_tables(grid_y, grid_z):
    cos_y, sin_y = rounded_tables(grid_y)
    cos_z, sin_z = rounded_tables(grid_z)
    chosen = half_plane(grid_y, grid_z)[0]
    rows, half = grid_y * grid_z, half_padded(grid_y, grid_z)
    width = 2 * half
    there = np.zeros((2, half, width), np.float32)
    there[0, : len(chosen), :rows] = (np.kron(cos_y, cos_z) - np.kron(sin_y, sin_z))[chosen]
    there[1, : len(chosen), :rows] = (np.kron(sin_y, cos_z) + np.kron(cos_y, sin_z))[chosen]
    back = there[:, :, :rows].transpose(2, 0, 1).reshape(rows, 2 * half)
    return np.concatenate([there.reshape(2 * half, width), back]).astype(ml_dtypes.bfloat16)


def plane_frequencies(grid_y, grid_z):
    chosen, opposite, differ = half_plane(grid_y, grid_z)
    table = np.zeros((half_padded(grid_y, grid_z), 8), np.float32)
    for column, (which, length) in enumerate(
        [
            (chosen // grid_z, grid_y),
            (chosen % grid_z, grid_z),
            (opposite // grid_z, grid_y),
            (opposite % grid_z, grid_z),
        ]
    ):
        table[: len(chosen), column] = np.where(which * 2 < length, which, which - length)
    table[: len(chosen), 4] = differ
    return table


def line_table(grid_x, sign):
    cosine, sine = rounded_tables(grid_x)
    re_in = np.concatenate([cosine, -sign * sine], axis=1)
    im_in = np.concatenate([sign * sine, cosine], axis=1)
    straight = np.concatenate([re_in, im_in], axis=0)
    turned = np.concatenate([sign * straight[:, grid_x:], -sign * straight[:, :grid_x]], axis=1)
    return np.concatenate([straight, turned], axis=1).astype(np.float32).astype(ml_dtypes.bfloat16)


def coulomb_kernel(grid, wavevectors, umklapp, frequencies, out):
    grid_x, grid_y, grid_z = grid
    width = out.shape[-1]
    cells = float(grid_x * grid_y * grid_z)
    k = lax.axis_index("ka")
    k_total = lax.axis_size("ka")

    def square(signed, length, shift):
        wavenumber = 2.0 * math.pi / (length * spacing) * (signed + shift)
        return wavenumber * wavenumber

    lane = lax.broadcasted_iota(jnp.int32, (1, width), 1)
    index_x = jnp.where(lane < grid_x, lane, lane - grid_x)
    signed_x = jnp.where(index_x * 2 < grid_x, index_x, index_x - grid_x).astype(jnp.float32)
    for s in range(out.shape[0]):
        visit = lax.rem(k + (k_total - s - 1), k_total)
        shift = [
            (wavevectors[a, k] - wavevectors[a, visit]).astype(jnp.float32) / KGRID
            + umklapp[0, s, a].astype(jnp.float32)
            for a in range(3)
        ]
        line = square(signed_x, grid_x, shift[0])
        kern = []
        for column in (0, 2):
            plane = square(frequencies[:, column : column + 1], grid_y, shift[1]) + square(
                frequencies[:, column + 1 : column + 2], grid_z, shift[2]
            )
            kern.append((4.0 * math.pi / cells) / (plane + line + screening_sq))
        opposite = kern[1] * frequencies[:, 4:5]
        out[s, 0] = kern[0] + opposite
        out[s, 1] = kern[0] - opposite


def coulomb(wavevectors, umklapp, grid_x, grid_y, grid_z):
    smem = pl.BlockSpec(memory_space=pltpu.SMEM)
    vmem = pl.BlockSpec(memory_space=pltpu.VMEM)
    half = half_padded(grid_y, grid_z)
    return pl.pallas_call(
        functools.partial(coulomb_kernel, (grid_x, grid_y, grid_z)),
        out_shape=jax.ShapeDtypeStruct((STEPS, 2, half, 2 * grid_x), jnp.float32),
        in_specs=[smem, smem, vmem],
        out_specs=vmem,
    )(wavevectors.T, umklapp, jnp.asarray(plane_frequencies(grid_y, grid_z)))


def exchange_kernel(
    visitors, psi, planes, lines, kern, out, dense, given, even, odd, pair, stack, plane
):
    rows, turn = out.shape[0], LANES // 2
    width = planes.shape[1]
    half = width // 2
    terms = STEPS * OCC_DEV
    left = lax.broadcasted_iota(jnp.int32, (1, LANES), 1) < turn
    chunk = 96

    def lanes(term):
        return pl.ds(term * LANES, LANES)

    given[:, pl.ds(rows, width - rows), :] = jnp.zeros(
        (2, width - rows, terms * LANES), given.dtype
    )
    for first in range(0, rows, chunk):
        own = psi[pl.ds(first, chunk), :].astype(jnp.float32)
        turned = pltpu.roll(own, turn, 1)
        with_phi = jnp.where(left, own, -turned)
        with_turned = jnp.where(left, turned, own)
        for term in range(terms):
            phi = visitors[term, pl.ds(first, chunk), :].astype(jnp.float32)
            density = phi * with_phi + pltpu.roll(phi, turn, 1) * with_turned
            dense[pl.ds(term * rows + first, chunk), :] = density.astype(jnp.bfloat16)
    for term in range(terms):
        both = jnp.dot(
            dense[pl.ds(term * rows, rows), :],
            lines[:, : 2 * LANES],
            preferred_element_type=jnp.float32,
        ).astype(jnp.bfloat16)
        given[0, pl.ds(0, rows), lanes(term)] = both[:, :LANES]
        given[1, pl.ds(0, rows), lanes(term)] = both[:, LANES:]

    even[...] = jnp.dot(planes[:half], given[0], preferred_element_type=jnp.float32)
    odd[...] = jnp.dot(planes[half:width], given[1], preferred_element_type=jnp.float32)
    for term in range(terms):
        total, differ = kern[term // OCC_DEV, 0], kern[term // OCC_DEV, 1]
        e, o = even[:, lanes(term)], odd[:, lanes(term)]
        pair[0, pl.ds(term * half, half), :] = (e * total + o * differ).astype(jnp.bfloat16)
        pair[1, pl.ds(term * half, half), :] = (e * differ + o * total).astype(jnp.bfloat16)
    for part in range(2):
        turned = jnp.dot(
            pair[part],
            lines[:, (2 + part) * LANES : (3 + part) * LANES],
            preferred_element_type=jnp.float32,
        ).astype(jnp.bfloat16)
        for term in range(terms):
            stack[pl.ds(part * half, half), lanes(term)] = turned[term * half : (term + 1) * half]

    plane[...] = jnp.dot(planes[width:], stack[...], preferred_element_type=jnp.float32)
    for first in range(0, rows, chunk):
        straight = crossed = None
        for term in range(terms):
            phi = visitors[term, pl.ds(first, chunk), :].astype(jnp.float32)
            potential = plane[pl.ds(first, chunk), lanes(term)]
            one, two = phi * potential, pltpu.roll(phi, turn, 1) * potential
            straight = one if term == 0 else straight + one
            crossed = two if term == 0 else crossed + two
        total = jnp.where(
            left, straight - pltpu.roll(straight, turn, 1), crossed + pltpu.roll(crossed, turn, 1)
        )
        out[pl.ds(first, chunk), :] = (prefactor * total).astype(out.dtype)


def apply_exchange(visitors, psi, kern, grid_x, grid_y, grid_z):
    rows = grid_y * grid_z
    terms = STEPS * OCC_DEV
    planes = plane_tables(grid_y, grid_z)
    lines = np.concatenate([line_table(grid_x, 1.0), line_table(grid_x, -1.0)], axis=1)
    width = planes.shape[1]
    half = width // 2
    vmem = pl.BlockSpec(memory_space=pltpu.VMEM)
    return pl.pallas_call(
        exchange_kernel,
        out_shape=jax.ShapeDtypeStruct((rows, LANES), jnp.bfloat16),
        in_specs=[vmem] * 5,
        out_specs=vmem,
        scratch_shapes=[
            pltpu.VMEM((terms * rows, LANES), jnp.bfloat16),
            pltpu.VMEM((2, width, terms * LANES), jnp.bfloat16),
            pltpu.VMEM((half, terms * LANES), jnp.float32),
            pltpu.VMEM((half, terms * LANES), jnp.float32),
            pltpu.VMEM((2, terms * half, LANES), jnp.bfloat16),
            pltpu.VMEM((2 * half, terms * LANES), jnp.bfloat16),
            pltpu.VMEM((rows, terms * LANES), jnp.float32),
        ],
        compiler_params=pltpu.CompilerParams(vmem_limit_bytes=16 * 1024 * 1024),
    )(
        visitors,
        psi,
        jnp.asarray(planes),
        jnp.asarray(lines),
        kern,
    )


def exchange(targets, occupied, wavevectors, umklapp, owners):
    resident = targets[0, 0]
    grid_y, grid_z, last_width = resident.shape
    grid_x = last_width // 2
    rows = grid_y * grid_z
    band = lax.axis_index("band")
    core, slot = band % 2, band // 16
    along_yz, cores = band_groups()
    n_yz = len(cores)

    flat = occupied[0].reshape(n_yz, OCC_DEV * rows // n_yz, last_width)
    spread = lax.all_to_all(flat, "band", 0, 0, tiled=True, axis_index_groups=along_yz)
    spread = lax.all_gather(spread, "band", axis_index_groups=cores)

    places = jnp.bitwise_and(owners[0], 1) * n_yz + lax.shift_right_logical(owners[0], 1)
    place = lax.dynamic_slice(places, (core, slot), (1, 1), allow_negative_indices=False)
    wanted = shift_ka_by_core(place, -1)
    spread = spread.reshape((2 * n_yz,) + flat.shape[1:])
    chosen = lax.dynamic_slice(
        spread, (wanted[0, 0], 0, 0), (1,) + flat.shape[1:], allow_negative_indices=False
    )[0]
    mine = shift_ka_by_core(chosen, 1)

    kern = coulomb(wavevectors, umklapp, grid_x, grid_y, grid_z)
    column = jnp.broadcast_to(mine[None], (n_yz,) + mine.shape)
    column = lax.all_to_all(column, "band", 0, 0, tiled=True, axis_index_groups=along_yz)
    visitors = lax.all_gather(column, "band", axis_index_groups=cores)
    visitors = visitors.reshape(STEPS * OCC_DEV, rows, last_width)

    result = apply_exchange(
        visitors,
        resident.reshape(rows, last_width),
        kern,
        grid_x,
        grid_y,
        grid_z,
    )
    return result.reshape((1, 1) + resident.shape)


def solution(mesh):
    placed = (
        P("ka", "band", None, None, None),
        P("ka", "band", None, None, None),
        P(),
        P("ka", None, None),
        P("ka", None, None),
    )
    return jax.shard_map(
        exchange,
        mesh=mesh,
        in_specs=placed,
        out_specs=P("ka", "band", None, None, None),
        check_vma=False,
    )
```

```python
import functools
import math

import jax
import jax.numpy as jnp
import ml_dtypes
import numpy as np
from jax import lax
from jax.experimental import pallas as pl
from jax.experimental.pallas import tpu as pltpu
from jax.sharding import PartitionSpec as P


OCC_DEV = 2
STEPS = 2
KGRID = 4

screening_sq = 0.16
spacing = 0.25
prefactor = -0.5

LANES = 128


def shift_ka_by_core(block, sign):
    n_ka, n_band = lax.axis_size("ka"), lax.axis_size("band")
    route = []
    for k in range(n_ka):
        for b in range(n_band):
            to = (k + sign * (1 + b % 2)) % n_ka
            route.append((k * n_band + b, to * n_band + b))
    return lax.ppermute(block, ("ka", "band"), route)


def band_groups():
    along_yz = [[yz * 2 + c for yz in range(16)] for c in range(2)]
    cores = [[yz * 2 + c for c in range(2)] for yz in range(16)]
    return along_yz, cores


def rounded_tables(length):
    indices = np.arange(length)
    angles = (indices[:, None] * indices[None, :] % length) * (2.0 * math.pi / length)
    rounded = lambda t: t.astype(np.float32).astype(ml_dtypes.bfloat16).astype(np.float64)
    return rounded(np.cos(angles)), rounded(np.sin(angles))


def half_plane(grid_y, grid_z):
    rows = np.arange(grid_y * grid_z)
    opposite = (-(rows // grid_z)) % grid_y * grid_z + (-(rows % grid_z)) % grid_z
    chosen = rows[rows <= opposite]
    return chosen, opposite[chosen], (opposite[chosen] != chosen).astype(np.float32)


def half_padded(grid_y, grid_z):
    return -(-len(half_plane(grid_y, grid_z)[0]) // 64) * 64


def plane_tables(grid_y, grid_z):
    cos_y, sin_y = rounded_tables(grid_y)
    cos_z, sin_z = rounded_tables(grid_z)
    chosen = half_plane(grid_y, grid_z)[0]
    rows, half = grid_y * grid_z, half_padded(grid_y, grid_z)
    width = 2 * half
    there = np.zeros((2, half, width), np.float32)
    there[0, : len(chosen), :rows] = (np.kron(cos_y, cos_z) - np.kron(sin_y, sin_z))[chosen]
    there[1, : len(chosen), :rows] = (np.kron(sin_y, cos_z) + np.kron(cos_y, sin_z))[chosen]
    back = there[:, :, :rows].transpose(2, 0, 1).reshape(rows, 2 * half)
    return np.concatenate([there.reshape(2 * half, width), back]).astype(ml_dtypes.bfloat16)


def plane_frequencies(grid_y, grid_z):
    chosen, opposite, differ = half_plane(grid_y, grid_z)
    table = np.zeros((half_padded(grid_y, grid_z), LANES), np.float32)
    for s in range(STEPS):
        for sign, rows in enumerate((chosen, opposite)):
            for axis, (which, length) in enumerate(((rows // grid_z, grid_y), (rows % grid_z, grid_z))):
                signed = np.where(which * 2 < length, which, which - length)
                table[: len(chosen), (axis * STEPS + s) * 2 + sign] = signed
    table[: len(chosen), 4 * STEPS] = differ
    return table


def line_table(grid_x, sign):
    cosine, sine = rounded_tables(grid_x)
    re_in = np.concatenate([cosine, -sign * sine], axis=1)
    im_in = np.concatenate([sign * sine, cosine], axis=1)
    straight = np.concatenate([re_in, im_in], axis=0)
    turned = np.concatenate([sign * straight[:, grid_x:], -sign * straight[:, :grid_x]], axis=1)
    return np.concatenate([straight, turned], axis=1).astype(np.float32).astype(ml_dtypes.bfloat16)


def wave_square(signed, length, shift):
    wavenumber = 2.0 * math.pi / (length * spacing) * (signed + shift)
    return wavenumber * wavenumber


def shifts_kernel(grid_x, wavevectors, umklapp, out):
    width = out.shape[-1]
    k = lax.axis_index("ka")
    k_total = lax.axis_size("ka")
    lane = lax.broadcasted_iota(jnp.int32, (1, width), 1)
    index_x = jnp.where(lane < grid_x, lane, lane - grid_x)
    signed_x = jnp.where(index_x * 2 < grid_x, index_x, index_x - grid_x).astype(jnp.float32)
    spread = jnp.zeros((1, width), jnp.float32)
    out[...] = jnp.zeros_like(out)
    for s in range(STEPS):
        visit = lax.rem(k + (k_total - s - 1), k_total)
        shift = [
            (wavevectors[a, k] - wavevectors[a, visit]).astype(jnp.float32) / KGRID
            + umklapp[0, s, a].astype(jnp.float32)
            for a in range(3)
        ]
        for axis in range(2):
            spread = jnp.where(lane // 2 == axis * STEPS + s, shift[1 + axis], spread)
        out[1 + s : 2 + s, :] = wave_square(signed_x, grid_x, shift[0]) + screening_sq
    out[0:1, :] = spread


def coulomb_shifts(wavevectors, umklapp, grid_x):
    smem = pl.BlockSpec(memory_space=pltpu.SMEM)
    return pl.pallas_call(
        functools.partial(shifts_kernel, grid_x),
        out_shape=jax.ShapeDtypeStruct((8, 2 * grid_x), jnp.float32),
        in_specs=[smem, smem],
        out_specs=pl.BlockSpec(memory_space=pltpu.VMEM),
    )(wavevectors.T, umklapp)


def exchange_kernel(
    grid, visitors, psi, planes, lines, frequencies, shifts, out, dense, given, even, odd, pair, stack, plane
):
    rows, turn = out.shape[0], LANES // 2
    width = planes.shape[1]
    half = width // 2
    terms = STEPS * OCC_DEV
    left = lax.broadcasted_iota(jnp.int32, (1, LANES), 1) < turn
    chunk = 96

    grid_x, grid_y, grid_z = grid
    cells = float(grid_x * grid_y * grid_z)
    lane = lax.broadcasted_iota(jnp.int32, (1, LANES), 1)
    length = jnp.where(lane < 2 * STEPS, float(grid_y), float(grid_z))

    def coulomb(s):
        squares = wave_square(frequencies[...], length, shifts[0:1, :])
        squares = squares + pltpu.roll(squares, LANES - 2 * STEPS, 1)
        kern = [
            (4.0 * math.pi / cells) / (squares[:, at : at + 1] + shifts[1 + s : 2 + s, :])
            for at in (2 * s, 2 * s + 1)
        ]
        opposite = kern[1] * frequencies[:, 4 * STEPS : 4 * STEPS + 1]
        return kern[0] + opposite, kern[0] - opposite

    def lanes(term):
        return pl.ds(term * LANES, LANES)

    given[:, pl.ds(rows, width - rows), :] = jnp.zeros(
        (2, width - rows, terms * LANES), given.dtype
    )
    for first in range(0, rows, chunk):
        own = psi[pl.ds(first, chunk), :].astype(jnp.float32)
        turned = pltpu.roll(own, turn, 1)
        with_phi = jnp.where(left, own, -turned)
        with_turned = jnp.where(left, turned, own)
        for term in range(terms):
            phi = visitors[term, pl.ds(first, chunk), :].astype(jnp.float32)
            density = phi * with_phi + pltpu.roll(phi, turn, 1) * with_turned
            dense[pl.ds(term * rows + first, chunk), :] = density.astype(jnp.bfloat16)
    for term in range(terms):
        both = jnp.dot(
            dense[pl.ds(term * rows, rows), :],
            lines[:, : 2 * LANES],
            preferred_element_type=jnp.float32,
        ).astype(jnp.bfloat16)
        given[0, pl.ds(0, rows), lanes(term)] = both[:, :LANES]
        given[1, pl.ds(0, rows), lanes(term)] = both[:, LANES:]

    even[...] = jnp.dot(planes[:half], given[0], preferred_element_type=jnp.float32)
    odd[...] = jnp.dot(planes[half:width], given[1], preferred_element_type=jnp.float32)
    for term in range(terms):
        if term % OCC_DEV == 0:
            total, differ = coulomb(term // OCC_DEV)
        e, o = even[:, lanes(term)], odd[:, lanes(term)]
        pair[0, pl.ds(term * half, half), :] = (e * total + o * differ).astype(jnp.bfloat16)
        pair[1, pl.ds(term * half, half), :] = (e * differ + o * total).astype(jnp.bfloat16)
    for part in range(2):
        turned = jnp.dot(
            pair[part],
            lines[:, (2 + part) * LANES : (3 + part) * LANES],
            preferred_element_type=jnp.float32,
        ).astype(jnp.bfloat16)
        for term in range(terms):
            stack[pl.ds(part * half, half), lanes(term)] = turned[term * half : (term + 1) * half]

    plane[...] = jnp.dot(planes[width:], stack[...], preferred_element_type=jnp.float32)
    for first in range(0, rows, chunk):
        straight = crossed = None
        for term in range(terms):
            phi = visitors[term, pl.ds(first, chunk), :].astype(jnp.float32)
            potential = plane[pl.ds(first, chunk), lanes(term)]
            one, two = phi * potential, pltpu.roll(phi, turn, 1) * potential
            straight = one if term == 0 else straight + one
            crossed = two if term == 0 else crossed + two
        total = jnp.where(
            left, straight - pltpu.roll(straight, turn, 1), crossed + pltpu.roll(crossed, turn, 1)
        )
        out[pl.ds(first, chunk), :] = (prefactor * total).astype(out.dtype)


def apply_exchange(visitors, psi, shifts, grid_x, grid_y, grid_z):
    rows = grid_y * grid_z
    terms = STEPS * OCC_DEV
    planes = plane_tables(grid_y, grid_z)
    lines = np.concatenate([line_table(grid_x, 1.0), line_table(grid_x, -1.0)], axis=1)
    width = planes.shape[1]
    half = width // 2
    vmem = pl.BlockSpec(memory_space=pltpu.VMEM)
    return pl.pallas_call(
        functools.partial(exchange_kernel, (grid_x, grid_y, grid_z)),
        out_shape=jax.ShapeDtypeStruct((rows, LANES), jnp.bfloat16),
        in_specs=[vmem] * 6,
        out_specs=vmem,
        scratch_shapes=[
            pltpu.VMEM((terms * rows, LANES), jnp.bfloat16),
            pltpu.VMEM((2, width, terms * LANES), jnp.bfloat16),
            pltpu.VMEM((half, terms * LANES), jnp.float32),
            pltpu.VMEM((half, terms * LANES), jnp.float32),
            pltpu.VMEM((2, terms * half, LANES), jnp.bfloat16),
            pltpu.VMEM((2 * half, terms * LANES), jnp.bfloat16),
            pltpu.VMEM((rows, terms * LANES), jnp.float32),
        ],
        compiler_params=pltpu.CompilerParams(vmem_limit_bytes=16 * 1024 * 1024),
    )(
        visitors,
        psi,
        jnp.asarray(planes),
        jnp.asarray(lines),
        jnp.asarray(plane_frequencies(grid_y, grid_z)),
        shifts,
    )


def exchange(targets, occupied, wavevectors, umklapp, owners):
    resident = targets[0, 0]
    grid_y, grid_z, last_width = resident.shape
    grid_x = last_width // 2
    rows = grid_y * grid_z
    band = lax.axis_index("band")
    core, slot = band % 2, band // 16
    along_yz, cores = band_groups()
    n_yz = len(cores)

    flat = occupied[0].reshape(n_yz, OCC_DEV * rows // n_yz, last_width)
    spread = lax.all_to_all(flat, "band", 0, 0, tiled=True, axis_index_groups=along_yz)
    spread = lax.all_gather(spread, "band", axis=1, axis_index_groups=cores)

    owner = lax.dynamic_slice(owners[0], (core, slot), (1, 1), allow_negative_indices=False)
    wanted = shift_ka_by_core(owner, -1)
    spread = spread.reshape((2 * n_yz,) + flat.shape[1:])
    chosen = lax.dynamic_slice(
        spread, (wanted[0, 0], 0, 0), (1,) + flat.shape[1:], allow_negative_indices=False
    )[0]
    mine = shift_ka_by_core(chosen, 1)

    shifts = coulomb_shifts(wavevectors, umklapp, grid_x)
    column = jnp.broadcast_to(mine[None], (n_yz,) + mine.shape)
    column = lax.all_to_all(column, "band", 0, 0, tiled=True, axis_index_groups=along_yz)
    visitors = lax.all_gather(column, "band", axis_index_groups=cores)
    visitors = visitors.reshape(STEPS * OCC_DEV, rows, last_width)

    result = apply_exchange(
        visitors,
        resident.reshape(rows, last_width),
        shifts,
        grid_x,
        grid_y,
        grid_z,
    )
    return result.reshape((1, 1) + resident.shape)


def solution(mesh):
    placed = (
        P("ka", "band", None, None, None),
        P("ka", "band", None, None, None),
        P(),
        P("ka", None, None),
        P("ka", None, None),
    )
    return jax.shard_map(
        exchange,
        mesh=mesh,
        in_specs=placed,
        out_specs=P("ka", "band", None, None, None),
        check_vma=False,
    )
```

```python
import functools
import math

import jax
import jax.numpy as jnp
import ml_dtypes
import numpy as np
from jax import lax
from jax.experimental import pallas as pl
from jax.experimental.pallas import tpu as pltpu
from jax.sharding import PartitionSpec as P


OCC_DEV = 2
STEPS = 2
KGRID = 4

screening_sq = 0.16
spacing = 0.25
prefactor = -0.5

LANES = 128


def shift_ka_by_core(block, sign):
    n_ka, n_band = lax.axis_size("ka"), lax.axis_size("band")
    route = []
    for k in range(n_ka):
        for b in range(n_band):
            to = (k + sign * (STEPS - b % 2)) % n_ka
            route.append((k * n_band + b, to * n_band + b))
    return lax.ppermute(block, ("ka", "band"), route)


def band_groups():
    along_yz = [[yz * 2 + c for yz in range(16)] for c in range(2)]
    cores = [[yz * 2 + c for c in range(2)] for yz in range(16)]
    return along_yz, cores


def rounded_tables(length):
    indices = np.arange(length)
    angles = (indices[:, None] * indices[None, :] % length) * (2.0 * math.pi / length)
    rounded = lambda t: t.astype(np.float32).astype(ml_dtypes.bfloat16).astype(np.float64)
    return rounded(np.cos(angles)), rounded(np.sin(angles))


def half_plane(grid_y, grid_z):
    rows = np.arange(grid_y * grid_z)
    opposite = (-(rows // grid_z)) % grid_y * grid_z + (-(rows % grid_z)) % grid_z
    chosen = rows[rows <= opposite]
    return chosen, opposite[chosen], (opposite[chosen] != chosen).astype(np.float32)


def half_padded(grid_y, grid_z):
    return -(-len(half_plane(grid_y, grid_z)[0]) // 64) * 64


def plane_tables(grid_y, grid_z):
    cos_y, sin_y = rounded_tables(grid_y)
    cos_z, sin_z = rounded_tables(grid_z)
    chosen = half_plane(grid_y, grid_z)[0]
    rows, half = grid_y * grid_z, half_padded(grid_y, grid_z)
    width = 2 * half
    there = np.zeros((2, half, width), np.float32)
    there[0, : len(chosen), :rows] = (np.kron(cos_y, cos_z) - np.kron(sin_y, sin_z))[chosen]
    there[1, : len(chosen), :rows] = (np.kron(sin_y, cos_z) + np.kron(cos_y, sin_z))[chosen]
    back = there[:, :, :rows].transpose(2, 0, 1).reshape(rows, 2 * half)
    return np.concatenate([there.reshape(2 * half, width), back]).astype(ml_dtypes.bfloat16)


def plane_frequencies(grid_y, grid_z):
    chosen, opposite, differ = half_plane(grid_y, grid_z)
    table = np.zeros((half_padded(grid_y, grid_z), LANES), np.float32)
    for s in range(STEPS):
        for sign, rows in enumerate((chosen, opposite)):
            for axis, (which, length) in enumerate(((rows // grid_z, grid_y), (rows % grid_z, grid_z))):
                signed = np.where(which * 2 < length, which, which - length)
                table[: len(chosen), (axis * STEPS + s) * 2 + sign] = signed
    table[: len(chosen), 4 * STEPS] = differ
    return table


def line_table(grid_x, sign):
    cosine, sine = rounded_tables(grid_x)
    re_in = np.concatenate([cosine, -sign * sine], axis=1)
    im_in = np.concatenate([sign * sine, cosine], axis=1)
    straight = np.concatenate([re_in, im_in], axis=0)
    turned = np.concatenate([sign * straight[:, grid_x:], -sign * straight[:, :grid_x]], axis=1)
    return np.concatenate([straight, turned], axis=1).astype(np.float32).astype(ml_dtypes.bfloat16)


def wave_square(signed, length, shift):
    wavenumber = 2.0 * math.pi / (length * spacing) * (signed + shift)
    return wavenumber * wavenumber


def shifts_kernel(grid_x, wavevectors, umklapp, out):
    width = out.shape[-1]
    k = lax.axis_index("ka")
    k_total = lax.axis_size("ka")
    lane = lax.broadcasted_iota(jnp.int32, (1, width), 1)
    index_x = jnp.where(lane < grid_x, lane, lane - grid_x)
    signed_x = jnp.where(index_x * 2 < grid_x, index_x, index_x - grid_x).astype(jnp.float32)
    spread = jnp.zeros((1, width), jnp.float32)
    out[...] = jnp.zeros_like(out)
    for s in range(STEPS):
        visit = lax.rem(k + (k_total - s - 1), k_total)
        shift = [
            (wavevectors[a, k] - wavevectors[a, visit]).astype(jnp.float32) / KGRID
            + umklapp[0, s, a].astype(jnp.float32)
            for a in range(3)
        ]
        for axis in range(2):
            spread = jnp.where(lane // 2 == axis * STEPS + s, shift[1 + axis], spread)
        out[1 + s : 2 + s, :] = wave_square(signed_x, grid_x, shift[0]) + screening_sq
    out[0:1, :] = spread


def coulomb_shifts(wavevectors, umklapp, grid_x):
    smem = pl.BlockSpec(memory_space=pltpu.SMEM)
    return pl.pallas_call(
        functools.partial(shifts_kernel, grid_x),
        out_shape=jax.ShapeDtypeStruct((8, 2 * grid_x), jnp.float32),
        in_specs=[smem, smem],
        out_specs=pl.BlockSpec(memory_space=pltpu.VMEM),
    )(wavevectors.T, umklapp)


def exchange_kernel(
    grid, visitors, psi, planes, lines, frequencies, shifts, out, dense, given, even, odd, pair, stack, plane
):
    rows, turn = out.shape[0], LANES // 2
    width = planes.shape[1]
    half = width // 2
    terms = STEPS * OCC_DEV
    left = lax.broadcasted_iota(jnp.int32, (1, LANES), 1) < turn
    chunk = 96

    grid_x, grid_y, grid_z = grid
    cells = float(grid_x * grid_y * grid_z)
    lane = lax.broadcasted_iota(jnp.int32, (1, LANES), 1)
    length = jnp.where(lane < 2 * STEPS, float(grid_y), float(grid_z))

    def coulomb(s):
        squares = wave_square(frequencies[...], length, shifts[0:1, :])
        squares = squares + pltpu.roll(squares, LANES - 2 * STEPS, 1)
        kern = [
            (4.0 * math.pi / cells) / (squares[:, at : at + 1] + shifts[1 + s : 2 + s, :])
            for at in (2 * s, 2 * s + 1)
        ]
        opposite = kern[1] * frequencies[:, 4 * STEPS : 4 * STEPS + 1]
        return kern[0] + opposite, kern[0] - opposite

    def lanes(term):
        return pl.ds(term * LANES, LANES)

    given[:, pl.ds(rows, width - rows), :] = jnp.zeros(
        (2, width - rows, terms * LANES), given.dtype
    )
    for first in range(0, rows, chunk):
        own = psi[pl.ds(first, chunk), :].astype(jnp.float32)
        turned = pltpu.roll(own, turn, 1)
        with_phi = jnp.where(left, own, -turned)
        with_turned = jnp.where(left, turned, own)
        for term in range(terms):
            phi = visitors[term, pl.ds(first, chunk), :].astype(jnp.float32)
            density = phi * with_phi + pltpu.roll(phi, turn, 1) * with_turned
            dense[pl.ds(term * rows + first, chunk), :] = density.astype(jnp.bfloat16)
    for term in range(terms):
        both = jnp.dot(
            dense[pl.ds(term * rows, rows), :],
            lines[:, : 2 * LANES],
            preferred_element_type=jnp.float32,
        ).astype(jnp.bfloat16)
        given[0, pl.ds(0, rows), lanes(term)] = both[:, :LANES]
        given[1, pl.ds(0, rows), lanes(term)] = both[:, LANES:]

    even[...] = jnp.dot(planes[:half], given[0], preferred_element_type=jnp.float32)
    odd[...] = jnp.dot(planes[half:width], given[1], preferred_element_type=jnp.float32)
    for term in range(terms):
        if term % OCC_DEV == 0:
            total, differ = coulomb(STEPS - 1 - term // OCC_DEV)
        e, o = even[:, lanes(term)], odd[:, lanes(term)]
        pair[0, pl.ds(term * half, half), :] = (e * total + o * differ).astype(jnp.bfloat16)
        pair[1, pl.ds(term * half, half), :] = (e * differ + o * total).astype(jnp.bfloat16)
    for part in range(2):
        turned = jnp.dot(
            pair[part],
            lines[:, (2 + part) * LANES : (3 + part) * LANES],
            preferred_element_type=jnp.float32,
        ).astype(jnp.bfloat16)
        for term in range(terms):
            stack[pl.ds(part * half, half), lanes(term)] = turned[term * half : (term + 1) * half]

    plane[...] = jnp.dot(planes[width:], stack[...], preferred_element_type=jnp.float32)
    for first in range(0, rows, chunk):
        straight = crossed = None
        for term in range(terms):
            phi = visitors[term, pl.ds(first, chunk), :].astype(jnp.float32)
            potential = plane[pl.ds(first, chunk), lanes(term)]
            one, two = phi * potential, pltpu.roll(phi, turn, 1) * potential
            straight = one if term == 0 else straight + one
            crossed = two if term == 0 else crossed + two
        total = jnp.where(
            left, straight - pltpu.roll(straight, turn, 1), crossed + pltpu.roll(crossed, turn, 1)
        )
        out[pl.ds(first, chunk), :] = (prefactor * total).astype(out.dtype)


def apply_exchange(visitors, psi, shifts, grid_x, grid_y, grid_z):
    rows = grid_y * grid_z
    terms = STEPS * OCC_DEV
    planes = plane_tables(grid_y, grid_z)
    lines = np.concatenate([line_table(grid_x, 1.0), line_table(grid_x, -1.0)], axis=1)
    width = planes.shape[1]
    half = width // 2
    vmem = pl.BlockSpec(memory_space=pltpu.VMEM)
    return pl.pallas_call(
        functools.partial(exchange_kernel, (grid_x, grid_y, grid_z)),
        out_shape=jax.ShapeDtypeStruct((rows, LANES), jnp.bfloat16),
        in_specs=[vmem] * 6,
        out_specs=vmem,
        scratch_shapes=[
            pltpu.VMEM((terms * rows, LANES), jnp.bfloat16),
            pltpu.VMEM((2, width, terms * LANES), jnp.bfloat16),
            pltpu.VMEM((half, terms * LANES), jnp.float32),
            pltpu.VMEM((half, terms * LANES), jnp.float32),
            pltpu.VMEM((2, terms * half, LANES), jnp.bfloat16),
            pltpu.VMEM((2 * half, terms * LANES), jnp.bfloat16),
            pltpu.VMEM((rows, terms * LANES), jnp.float32),
        ],
        compiler_params=pltpu.CompilerParams(vmem_limit_bytes=16 * 1024 * 1024),
    )(
        visitors,
        psi,
        jnp.asarray(planes),
        jnp.asarray(lines),
        jnp.asarray(plane_frequencies(grid_y, grid_z)),
        shifts,
    )


def exchange(targets, occupied, wavevectors, umklapp, owners):
    resident = targets[0, 0]
    grid_y, grid_z, last_width = resident.shape
    grid_x = last_width // 2
    rows = grid_y * grid_z
    band = lax.axis_index("band")
    core, slot = band % 2, band // 16
    along_yz, cores = band_groups()
    n_yz = len(cores)

    flat = occupied[0].reshape(n_yz, OCC_DEV * rows // n_yz, last_width)
    spread = lax.all_to_all(flat, "band", 0, 0, tiled=True, axis_index_groups=along_yz)
    spread = lax.all_gather(spread, "band", axis=1, axis_index_groups=cores)

    owner = lax.dynamic_slice(owners[0], (1 - core, slot), (1, 1), allow_negative_indices=False)
    wanted = shift_ka_by_core(owner, -1)
    spread = spread.reshape((2 * n_yz,) + flat.shape[1:])
    chosen = lax.dynamic_slice(
        spread, (wanted[0, 0], 0, 0), (1,) + flat.shape[1:], allow_negative_indices=False
    )[0]
    mine = shift_ka_by_core(chosen, 1)

    shifts = coulomb_shifts(wavevectors, umklapp, grid_x)
    column = jnp.broadcast_to(mine[None], (n_yz,) + mine.shape)
    column = lax.all_to_all(column, "band", 0, 0, tiled=True, axis_index_groups=along_yz)
    visitors = lax.all_gather(column, "band", axis_index_groups=cores)
    visitors = visitors.reshape(STEPS * OCC_DEV, rows, last_width)

    result = apply_exchange(
        visitors,
        resident.reshape(rows, last_width),
        shifts,
        grid_x,
        grid_y,
        grid_z,
    )
    return result.reshape((1, 1) + resident.shape)


def solution(mesh):
    placed = (
        P("ka", "band", None, None, None),
        P("ka", "band", None, None, None),
        P(),
        P("ka", None, None),
        P("ka", None, None),
    )
    return jax.shard_map(
        exchange,
        mesh=mesh,
        in_specs=placed,
        out_specs=P("ka", "band", None, None, None),
        check_vma=False,
    )
```

```python
import functools
import math

import jax
import jax.numpy as jnp
import ml_dtypes
import numpy as np
from jax import lax
from jax.experimental import pallas as pl
from jax.experimental.pallas import tpu as pltpu
from jax.sharding import PartitionSpec as P


OCC_DEV = 2
STEPS = 2
KGRID = 4

screening_sq = 0.16
spacing = 0.25
prefactor = -0.5

LANES = 128


def shift_ka_by_core(block, sign):
    n_ka, n_band = lax.axis_size("ka"), lax.axis_size("band")
    route = []
    for k in range(n_ka):
        for b in range(n_band):
            to = (k + sign * (STEPS - b % 2)) % n_ka
            route.append((k * n_band + b, to * n_band + b))
    return lax.ppermute(block, ("ka", "band"), route)


def band_groups():
    along_yz = [[yz * 2 + c for yz in range(16)] for c in range(2)]
    cores = [[yz * 2 + c for c in range(2)] for yz in range(16)]
    return along_yz, cores


def rounded_tables(length):
    indices = np.arange(length)
    angles = (indices[:, None] * indices[None, :] % length) * (2.0 * math.pi / length)
    rounded = lambda t: t.astype(np.float32).astype(ml_dtypes.bfloat16).astype(np.float64)
    return rounded(np.cos(angles)), rounded(np.sin(angles))


def half_plane(grid_y, grid_z):
    rows = np.arange(grid_y * grid_z)
    opposite = (-(rows // grid_z)) % grid_y * grid_z + (-(rows % grid_z)) % grid_z
    chosen = rows[rows <= opposite]
    return chosen, opposite[chosen], (opposite[chosen] != chosen).astype(np.float32)


def half_padded(grid_y, grid_z):
    return -(-len(half_plane(grid_y, grid_z)[0]) // 64) * 64


def plane_tables(grid_y, grid_z):
    cos_y, sin_y = rounded_tables(grid_y)
    cos_z, sin_z = rounded_tables(grid_z)
    chosen = half_plane(grid_y, grid_z)[0]
    rows, half = grid_y * grid_z, half_padded(grid_y, grid_z)
    width = 2 * half
    there = np.zeros((2, half, width), np.float32)
    there[0, : len(chosen), :rows] = (np.kron(cos_y, cos_z) - np.kron(sin_y, sin_z))[chosen]
    there[1, : len(chosen), :rows] = (np.kron(sin_y, cos_z) + np.kron(cos_y, sin_z))[chosen]
    back = there[:, :, :rows].transpose(2, 0, 1).reshape(rows, 2 * half)
    return np.concatenate([there.reshape(2 * half, width), back]).astype(ml_dtypes.bfloat16)


def plane_frequencies(grid_y, grid_z):
    chosen, opposite, differ = half_plane(grid_y, grid_z)
    table = np.zeros((half_padded(grid_y, grid_z), LANES), np.float32)
    for s in range(STEPS):
        for sign, rows in enumerate((chosen, opposite)):
            for axis, (which, length) in enumerate(((rows // grid_z, grid_y), (rows % grid_z, grid_z))):
                signed = np.where(which * 2 < length, which, which - length)
                table[: len(chosen), (axis * STEPS + s) * 2 + sign] = signed
    table[: len(chosen), 4 * STEPS] = differ
    return table


def line_table(grid_x, sign):
    cosine, sine = rounded_tables(grid_x)
    re_in = np.concatenate([cosine, -sign * sine], axis=1)
    im_in = np.concatenate([sign * sine, cosine], axis=1)
    straight = np.concatenate([re_in, im_in], axis=0)
    turned = np.concatenate([sign * straight[:, grid_x:], -sign * straight[:, :grid_x]], axis=1)
    return np.concatenate([straight, turned], axis=1).astype(np.float32).astype(ml_dtypes.bfloat16)


def wave_square(signed, length, shift):
    wavenumber = 2.0 * math.pi / (length * spacing) * (signed + shift)
    return wavenumber * wavenumber


def shifts_kernel(grid_x, wavevectors, umklapp, out):
    width = out.shape[-1]
    k = lax.axis_index("ka")
    k_total = lax.axis_size("ka")
    lane = lax.broadcasted_iota(jnp.int32, (1, width), 1)
    index_x = jnp.where(lane < grid_x, lane, lane - grid_x)
    signed_x = jnp.where(index_x * 2 < grid_x, index_x, index_x - grid_x).astype(jnp.float32)
    spread = jnp.zeros((1, width), jnp.float32)
    out[...] = jnp.zeros_like(out)
    for s in range(STEPS):
        visit = lax.rem(k + (k_total - s - 1), k_total)
        shift = [
            (wavevectors[a, k] - wavevectors[a, visit]).astype(jnp.float32) / KGRID
            + umklapp[0, s, a].astype(jnp.float32)
            for a in range(3)
        ]
        for axis in range(2):
            spread = jnp.where(lane // 2 == axis * STEPS + s, shift[1 + axis], spread)
        out[1 + s : 2 + s, :] = wave_square(signed_x, grid_x, shift[0]) + screening_sq
    out[0:1, :] = spread


def coulomb_shifts(wavevectors, umklapp, grid_x):
    smem = pl.BlockSpec(memory_space=pltpu.SMEM)
    return pl.pallas_call(
        functools.partial(shifts_kernel, grid_x),
        out_shape=jax.ShapeDtypeStruct((8, 2 * grid_x), jnp.float32),
        in_specs=[smem, smem],
        out_specs=pl.BlockSpec(memory_space=pltpu.VMEM),
    )(wavevectors.T, umklapp)


def exchange_kernel(
    grid, visitors, psi, planes, lines, frequencies, shifts, out, dense, given, even, odd, pair, stack, plane
):
    rows, turn = out.shape[0], LANES // 2
    width = planes.shape[1]
    half = width // 2
    terms = STEPS * OCC_DEV
    left = lax.broadcasted_iota(jnp.int32, (1, LANES), 1) < turn
    chunk = 96

    grid_x, grid_y, grid_z = grid
    cells = float(grid_x * grid_y * grid_z)
    lane = lax.broadcasted_iota(jnp.int32, (1, LANES), 1)
    length = jnp.where(lane < 2 * STEPS, float(grid_y), float(grid_z))

    def coulomb(s):
        squares = wave_square(frequencies[...], length, shifts[0:1, :])
        squares = squares + pltpu.roll(squares, LANES - 2 * STEPS, 1)
        kern = [
            (4.0 * math.pi / cells) / (squares[:, at : at + 1] + shifts[1 + s : 2 + s, :])
            for at in (2 * s, 2 * s + 1)
        ]
        opposite = kern[1] * frequencies[:, 4 * STEPS : 4 * STEPS + 1]
        return kern[0] + opposite, kern[0] - opposite

    def lanes(term):
        return pl.ds(term * LANES, LANES)

    given[:, pl.ds(rows, width - rows), :] = jnp.zeros(
        (2, width - rows, terms * LANES), given.dtype
    )
    for first in range(0, rows, chunk):
        own = psi[pl.ds(first, chunk), :].astype(jnp.float32)
        turned = pltpu.roll(own, turn, 1)
        with_phi = jnp.where(left, own, -turned)
        with_turned = jnp.where(left, turned, own)
        for term in range(terms):
            phi = visitors[term, pl.ds(first, chunk), :]
            other = pltpu.roll(phi, turn, 1).astype(jnp.float32)
            density = phi.astype(jnp.float32) * with_phi + other * with_turned
            dense[pl.ds(term * rows + first, chunk), :] = density.astype(jnp.bfloat16)
    for term in range(terms):
        both = jnp.dot(
            dense[pl.ds(term * rows, rows), :],
            lines[:, : 2 * LANES],
            preferred_element_type=jnp.float32,
        ).astype(jnp.bfloat16)
        given[0, pl.ds(0, rows), lanes(term)] = both[:, :LANES]
        given[1, pl.ds(0, rows), lanes(term)] = both[:, LANES:]

    even[...] = jnp.dot(planes[:half], given[0], preferred_element_type=jnp.float32)
    odd[...] = jnp.dot(planes[half:width], given[1], preferred_element_type=jnp.float32)
    for term in range(terms):
        if term % OCC_DEV == 0:
            total, differ = coulomb(STEPS - 1 - term // OCC_DEV)
        e, o = even[:, lanes(term)], odd[:, lanes(term)]
        pair[0, pl.ds(term * half, half), :] = (e * total + o * differ).astype(jnp.bfloat16)
        pair[1, pl.ds(term * half, half), :] = (e * differ + o * total).astype(jnp.bfloat16)
    for part in range(2):
        turned = jnp.dot(
            pair[part],
            lines[:, (2 + part) * LANES : (3 + part) * LANES],
            preferred_element_type=jnp.float32,
        ).astype(jnp.bfloat16)
        for term in range(terms):
            stack[pl.ds(part * half, half), lanes(term)] = turned[term * half : (term + 1) * half]

    plane[...] = jnp.dot(planes[width:], stack[...], preferred_element_type=jnp.float32)
    for first in range(0, rows, chunk):
        straight = crossed = None
        for term in range(terms):
            phi = visitors[term, pl.ds(first, chunk), :]
            other = pltpu.roll(phi, turn, 1).astype(jnp.float32)
            potential = plane[pl.ds(first, chunk), lanes(term)]
            one, two = phi.astype(jnp.float32) * potential, other * potential
            straight = one if term == 0 else straight + one
            crossed = two if term == 0 else crossed + two
        total = jnp.where(
            left, straight - pltpu.roll(straight, turn, 1), crossed + pltpu.roll(crossed, turn, 1)
        )
        out[pl.ds(first, chunk), :] = (prefactor * total).astype(out.dtype)


def apply_exchange(visitors, psi, shifts, grid_x, grid_y, grid_z):
    rows = grid_y * grid_z
    terms = STEPS * OCC_DEV
    planes = plane_tables(grid_y, grid_z)
    lines = np.concatenate([line_table(grid_x, 1.0), line_table(grid_x, -1.0)], axis=1)
    width = planes.shape[1]
    half = width // 2
    vmem = pl.BlockSpec(memory_space=pltpu.VMEM)
    return pl.pallas_call(
        functools.partial(exchange_kernel, (grid_x, grid_y, grid_z)),
        out_shape=jax.ShapeDtypeStruct((rows, LANES), jnp.bfloat16),
        in_specs=[vmem] * 6,
        out_specs=vmem,
        scratch_shapes=[
            pltpu.VMEM((terms * rows, LANES), jnp.bfloat16),
            pltpu.VMEM((2, width, terms * LANES), jnp.bfloat16),
            pltpu.VMEM((half, terms * LANES), jnp.float32),
            pltpu.VMEM((half, terms * LANES), jnp.float32),
            pltpu.VMEM((2, terms * half, LANES), jnp.bfloat16),
            pltpu.VMEM((2 * half, terms * LANES), jnp.bfloat16),
            pltpu.VMEM((rows, terms * LANES), jnp.float32),
        ],
        compiler_params=pltpu.CompilerParams(vmem_limit_bytes=16 * 1024 * 1024),
    )(
        visitors,
        psi,
        jnp.asarray(planes),
        jnp.asarray(lines),
        jnp.asarray(plane_frequencies(grid_y, grid_z)),
        shifts,
    )


def exchange(targets, occupied, wavevectors, umklapp, owners):
    resident = targets[0, 0]
    grid_y, grid_z, last_width = resident.shape
    grid_x = last_width // 2
    rows = grid_y * grid_z
    band = lax.axis_index("band")
    core, slot = band % 2, band // 16
    along_yz, cores = band_groups()
    n_yz = len(cores)

    flat = occupied[0].reshape(n_yz, OCC_DEV * rows // n_yz, last_width)
    spread = lax.all_to_all(flat, "band", 0, 0, tiled=True, axis_index_groups=along_yz)
    spread = lax.all_gather(spread, "band", axis=1, axis_index_groups=cores)

    owner = lax.dynamic_slice(owners[0], (1 - core, slot), (1, 1), allow_negative_indices=False)
    wanted = shift_ka_by_core(owner, -1)
    spread = spread.reshape((2 * n_yz,) + flat.shape[1:])
    chosen = lax.dynamic_slice(
        spread, (wanted[0, 0], 0, 0), (1,) + flat.shape[1:], allow_negative_indices=False
    )[0]
    mine = shift_ka_by_core(chosen, 1)

    shifts = coulomb_shifts(wavevectors, umklapp, grid_x)
    column = jnp.broadcast_to(mine[None], (n_yz,) + mine.shape)
    column = lax.all_to_all(column, "band", 0, 0, tiled=True, axis_index_groups=along_yz)
    visitors = lax.all_gather(column, "band", axis_index_groups=cores)
    visitors = visitors.reshape(STEPS * OCC_DEV, rows, last_width)

    result = apply_exchange(
        visitors,
        resident.reshape(rows, last_width),
        shifts,
        grid_x,
        grid_y,
        grid_z,
    )
    return result.reshape((1, 1) + resident.shape)


def solution(mesh):
    placed = (
        P("ka", "band", None, None, None),
        P("ka", "band", None, None, None),
        P(),
        P("ka", None, None),
        P("ka", None, None),
    )
    return jax.shard_map(
        exchange,
        mesh=mesh,
        in_specs=placed,
        out_specs=P("ka", "band", None, None, None),
        check_vma=False,
    )
```
